256 devices in a mesh: sub: 2 (over z), row: 128 (over y, x, core).
Axes of the slice: x: 8, y: 8, z: 2, core: 2. Of those that a mesh axis runs over, the one named last changes fastest.
The devices are a block of a 8x8x16 slice.
Arguments:
- diag_blocks: float32 [4096, 128, 128], P(('sub', 'row')), parts along dimension 0, may hold values from -0.05 to 16, as said below
- coupling: float32 [4096, 3, 128, 128], P(('sub', 'row')), parts along dimension 0, may hold values from -0.05 to 0.05
- offsets: int32 [4096, 3], P(('sub', 'row')), parts along dimension 0, may hold values from 1 to 4, as said below
- mass: float32 [524288], P(('sub', 'row')), parts along dimension 0, may hold values from 0.5 to 2
- initial_modes: float32 [32, 524288], P(None, ('sub', 'row')), parts along dimension 1, may hold values from -6 to 6
Outputs:
- mass_density: float32 [524288], P(('sub', 'row')), parts along dimension 0
- energy_density: float32 [524288], P(('sub', 'row')), parts along dimension 0
The draws below stay inside these ranges and needn't reach their ends.
There are 2 independent parts, one for each index of `sub`. The reference program is written for one: setup_inputs(seed, part) draws one part's arguments, and reference() takes and returns one part's arrays. A program takes and returns all parts, laid end to end along the dimension named above; each array names one. Nothing has to cross between parts.
Inputs may be any that keep to these rules, and one draw needn't show every extreme that they name: `diag_blocks`: each block is symmetric; entries off a block's diagonal lie in -0.05 to 0.05, its diagonal entries in 1 to 16. The 3 offsets of a block row are distinct.
All inputs are finite; a program needn't handle non-finite values.
Results may differ from the reference program's by a relative error of at most 0.0003.
Values sent between devices are 32-bit elements; how exact they have to be, the bound alone decides.
A program may use at most 128 MiB of HBM per device.

```python
import math
import jax
import jax.numpy as jnp
from jax import lax

BLK = 128
MODES = 32
SLOTS = 3
REACH = 4
ITERS = 3
PURIFY = 28
NBLK = 2048
N = 262144


def draw_diag_blocks(key, part):
    key_off, key_diag = jax.random.split(key)
    shape = (NBLK, BLK, BLK)
    couplings = jax.random.uniform(key_off, shape, jnp.float32, -0.05, 0.05)
    diagonal = jnp.exp(jax.random.uniform(key_diag, (NBLK, BLK), jnp.float32, 0.0, jnp.log(10.0)))
    identity = jnp.eye(BLK, dtype=jnp.float32)
    symmetric = 0.5 * (couplings + jnp.swapaxes(couplings, 1, 2))
    return symmetric * (1.0 - identity)[None, :, :] + identity[None, :, :] * diagonal[:, :, None]


def draw_offsets(key, part):
    scores = jax.random.randint(key, (NBLK, REACH), 0, 1 << 20) * REACH + jnp.arange(REACH, dtype=jnp.int32)[None, :]
    ranking = jnp.argsort(scores, axis=1)
    return (ranking[:, :SLOTS] + 1).astype(jnp.int32)


def steps_of(key, extent, cuts, smallest, largest):
    gain, own = 1.0, jax.random.fold_in(key, 6)
    for axis_at, blocks in cuts:
        steps = jnp.exp(jax.random.uniform(jax.random.fold_in(own, axis_at), (blocks,), jnp.float32, smallest / len(cuts), largest / len(cuts)))
        gain = gain * jnp.repeat(steps, extent[axis_at] // blocks).reshape([-1 if axis == axis_at else 1 for axis in range(len(extent))])
    return gain


def gaussian(own_key, dims, deviation, limit, pieces=(), held_as=jnp.bfloat16):
    entries = jax.random.normal(own_key, dims, jnp.float32) * deviation
    if len(pieces) > 0:
        entries = steps_of(own_key, dims, pieces, -0.22, 0.18) * entries
    return jnp.clip(entries, min=-limit, max=limit).astype(held_as)


def setup_inputs(seed: int = 0, part: int = 0) -> dict:
    arg_keys = jax.random.split(jax.random.key(seed), 6)
    part_splits = jax.random.split(jax.random.fold_in(arg_keys[5], part), 6)
    diag_blocks = draw_diag_blocks(jax.random.fold_in(jax.random.fold_in(arg_keys[5], part), 71), part)
    coupling = jnp.clip(jax.random.uniform(part_splits[1], (NBLK, SLOTS, BLK, BLK), jnp.float32, -0.05, 0.05) * steps_of(part_splits[1], (NBLK, SLOTS, BLK, BLK), ((0, 128),), -0.4, 0.0), -0.05, 0.05)
    offsets = draw_offsets(jax.random.fold_in(jax.random.fold_in(arg_keys[5], part), 71), part)
    mass = jnp.clip(jnp.exp(math.log(2.0) - 1.3862944 * jax.random.uniform(part_splits[3], (N,), jnp.float32) ** steps_of(part_splits[3], (N,), ((0, 128),), -0.2, 0.2)), 0.5, 2.0)
    initial_modes = gaussian(part_splits[4], (MODES, N), 1.0, 6.0, ((1, 128),), jnp.float32)
    return {"diag_blocks": diag_blocks, "coupling": coupling, "offsets": offsets, "mass": mass, "initial_modes": initial_modes}


PRECISE = lax.Precision.HIGHEST

def stiffness_apply(vectors, diag_blocks, coupling, offsets):
    rowcount = vectors.shape[0]
    block_count = diag_blocks.shape[0]
    block_width = diag_blocks.shape[1]
    blocked = vectors.reshape(rowcount, block_count, block_width)
    result = jnp.einsum('nbk,bkj->nbj', blocked, diag_blocks, precision=PRECISE)
    targets = jnp.arange(block_count, dtype=jnp.int32)[:, None] - offsets
    present = (targets >= 0).astype(vectors.dtype)
    clipped = jnp.maximum(targets, 0).astype(jnp.int32)
    gathered = blocked[:, clipped, :] * present[None, :, :, None]
    result = result + jnp.einsum('nbsk,bsjk->nbj', gathered, coupling, precision=PRECISE)
    products = jnp.einsum('nbk,bskj->nbsj', blocked, coupling, precision=PRECISE) * present[None, :, :, None]
    result = result.at[:, clipped, :].add(products)
    return result.reshape(rowcount, block_count * block_width)

def purify(matrix, occupied, steps_count):
    order = matrix.shape[0]
    identity = jnp.eye(order, dtype=matrix.dtype)
    diagonal = jnp.diagonal(matrix)
    center = jnp.sum(diagonal) / order
    radius = lax.optimization_barrier(jnp.sum(jnp.abs(matrix), axis=1)) - jnp.abs(diagonal)
    highest = jnp.max(diagonal + radius)
    lowest = jnp.min(diagonal - radius)
    factor = jnp.minimum(occupied / jnp.maximum(highest - center, 1e-06), (order - occupied) / jnp.maximum(center - lowest, 1e-06))
    initial = factor / order * (center * identity - matrix) + occupied / order * identity

    def purify_step(index, density):
        square = jnp.dot(density, density, precision=PRECISE)
        cube = jnp.dot(square, density, precision=PRECISE)
        numerator = jnp.trace(square - cube)
        denominator = jnp.trace(density - square)
        safe_denominator = jnp.where(jnp.abs(denominator) > 1e-12, denominator, 1.0)
        ratio = jnp.clip(numerator / safe_denominator, 0.0, 1.0)
        upward = ((1.0 + ratio) * square - cube) / jnp.maximum(ratio, 0.5)
        downward = ((1.0 - 2.0 * ratio) * density + (1.0 + ratio) * square - cube) / jnp.maximum(1.0 - ratio, 0.5)
        return jnp.where(ratio >= 0.5, upward, downward)
    return lax.fori_loop(0, steps_count, purify_step, initial)

def ritz_basis(gram_stiff, gram_mass, modes_wanted, steps_count):
    order = gram_stiff.shape[0]
    gram_stiff = 0.5 * (gram_stiff + gram_stiff.T)
    gram_mass = 0.5 * (gram_mass + gram_mass.T)
    scaling = lax.rsqrt(jnp.diagonal(gram_mass) + 1e-06)
    stiff_scaled = scaling[:, None] * gram_stiff * scaling[None, :]
    mass_scaled = scaling[:, None] * gram_mass * scaling[None, :]
    factor_low = jnp.linalg.cholesky(mass_scaled)
    identity = jnp.eye(order, dtype=gram_stiff.dtype)
    inverse_low = lax.linalg.triangular_solve(factor_low, identity, left_side=True, lower=True)
    reduced = jnp.dot(jnp.dot(inverse_low, stiff_scaled, precision=PRECISE), inverse_low.T, precision=PRECISE)
    reduced = 0.5 * (reduced + reduced.T)
    if order > modes_wanted:
        projector = purify(reduced, modes_wanted, steps_count)
        columns = projector[:, :modes_wanted]
    else:
        columns = identity
    correlation = jnp.dot(columns.T, columns, precision=PRECISE)
    correlation_low = jnp.linalg.cholesky(correlation)
    orthonormal = lax.linalg.triangular_solve(correlation_low, columns.T, left_side=True, lower=True).T
    coefficients = scaling[:, None] * jnp.dot(inverse_low.T, orthonormal, precision=PRECISE)
    projected = jnp.dot(jnp.dot(orthonormal.T, reduced, precision=PRECISE), orthonormal, precision=PRECISE)
    return (coefficients, 0.5 * (projected + projected.T))

def reference(diag_blocks, coupling, offsets, mass, initial_modes):
    stiff_diag = jnp.diagonal(diag_blocks, axis1=1, axis2=2).reshape(-1)

    def gram_pair(basis, stiff_basis):
        gram_stiff = jnp.dot(basis, stiff_basis.T, precision=PRECISE)
        gram_mass = jnp.dot(basis * mass[None, :], basis.T, precision=PRECISE)
        return (gram_stiff, gram_mass)
    stiff_initial = stiffness_apply(initial_modes, diag_blocks, coupling, offsets)
    gram_stiff, gram_mass = gram_pair(initial_modes, stiff_initial)
    coefficients, projected = ritz_basis(gram_stiff, gram_mass, MODES, PURIFY)
    modes_now = jnp.dot(coefficients.T, initial_modes, precision=PRECISE)
    stiff_modes = jnp.dot(coefficients.T, stiff_initial, precision=PRECISE)
    directions = None
    stiff_directions = None
    for iteration in range(ITERS):
        residual = stiff_modes - jnp.dot(projected, modes_now * mass[None, :], precision=PRECISE)
        precond = residual / stiff_diag[None, :]
        stiff_precond = stiffness_apply(precond, diag_blocks, coupling, offsets)
        if directions is None:
            basis = jnp.concatenate([modes_now, precond], axis=0)
            stiff_basis = jnp.concatenate([stiff_modes, stiff_precond], axis=0)
        else:
            basis = jnp.concatenate([modes_now, precond, directions], axis=0)
            stiff_basis = jnp.concatenate([stiff_modes, stiff_precond, stiff_directions], axis=0)
        gram_stiff, gram_mass = gram_pair(basis, stiff_basis)
        coefficients, projected = ritz_basis(gram_stiff, gram_mass, MODES, PURIFY)
        directions = jnp.dot(coefficients[MODES:].T, basis[MODES:], precision=PRECISE)
        stiff_directions = jnp.dot(coefficients[MODES:].T, stiff_basis[MODES:], precision=PRECISE)
        modes_now = jnp.dot(coefficients.T, basis, precision=PRECISE)
        stiff_modes = jnp.dot(coefficients.T, stiff_basis, precision=PRECISE)
    weight = modes_now.shape[1] / MODES
    mass_density = weight * mass * lax.optimization_barrier(jnp.sum(modes_now * modes_now, axis=0))
    energy_density = weight * lax.optimization_barrier(jnp.sum(modes_now * stiff_modes, axis=0))
    return (mass_density, energy_density)
```

```python
import jax
import jax.numpy as jnp
from jax import lax
from jax.experimental import pallas as pl
from jax.experimental.pallas import tpu as pltpu
from jax.sharding import PartitionSpec as P

MODES = 32
REACH = 4
SLOTS = 3
ITERS = 3
PURIFY = 28
WIDTH = 128
TORUS = (8, 8, 2)
MESH = pl.DeviceIdType.MESH

HIGH = lax.Precision.HIGH
HIGHEST = lax.Precision.HIGHEST


def mm(a, b, precision):
    return lax.dot_general(
        a, b, (((1,), (0,)), ((), ())), precision=precision, preferred_element_type=jnp.float32
    )


def mm_nt(a, b, precision):
    return lax.dot_general(
        a, b, (((1,), (1,)), ((), ())), precision=precision, preferred_element_type=jnp.float32
    )


def lanes(shape):
    return lax.broadcasted_iota(jnp.int32, shape, 1)


def sublanes(shape):
    return lax.broadcasted_iota(jnp.int32, shape, 0)


def eye(n):
    return (sublanes((n, n)) == lanes((n, n))).astype(jnp.float32)


def total(x):
    return jnp.sum(jnp.sum(x, axis=0, keepdims=True), axis=1, keepdims=True)


def inverse_factor(table, first):
    rows, cols = table.shape
    done = []
    for start in range(0, rows, 8):
        live = table.shape[0]
        column = [
            jnp.broadcast_to(table[:, first + start + k : first + start + k + 1], (live, cols))
            for k in range(8)
        ]
        index = sublanes((live, cols))
        lane = lanes((live, cols))
        for k in range(8):
            at = first + start + k
            pivot = column[k][k : k + 1, :]
            scale = lax.rsqrt(pivot)
            row = jnp.where(lane[0:1] == at, 1.0, table[k : k + 1, :]) * scale
            factor = jnp.where(index > k, column[k] * scale, 0.0)
            table = jnp.where((index > k) & (lane == at), 0.0, table) - factor * row
            table = jnp.where(index == k, row, table)
            for m in range(k + 1, 8):
                column[m] = column[m] - factor * (column[m][k : k + 1, :] * scale)
        done.append(table[:8])
        table = table[8:]
    result = jnp.concatenate(done, axis=0) if len(done) > 1 else done[0]
    shape = (rows, cols)
    return jnp.where(lanes(shape) <= sublanes(shape) + first, result, 0.0)


def purify(matrix):
    n = matrix.shape[0]
    identity = eye(n)
    diagonal = jnp.sum(matrix * identity, axis=0, keepdims=True)
    radius = jnp.sum(jnp.abs(matrix), axis=0, keepdims=True) - jnp.abs(diagonal)
    center = jnp.sum(diagonal, axis=1, keepdims=True) / n
    highest = jnp.max(diagonal + radius, axis=1, keepdims=True)
    lowest = jnp.min(diagonal - radius, axis=1, keepdims=True)
    factor = jnp.minimum(
        MODES / jnp.maximum(highest - center, 1e-6), (n - MODES) / jnp.maximum(center - lowest, 1e-6)
    )
    initial = factor / n * (center * identity - matrix) + MODES / n * identity

    def step(index, density):
        square = mm(density, density, HIGHEST)
        cube = mm(square, density, HIGHEST)
        denominator = total((density - square) * identity)
        numerator = total(square * (identity - density))
        safe = jnp.where(jnp.abs(denominator) > 1e-12, denominator, 1.0)
        ratio = jnp.clip(numerator / safe, 0.0, 1.0)
        up = ratio >= 0.5
        scale = 1.0 / jnp.maximum(jnp.where(up, ratio, 1.0 - ratio), 0.5)
        first = jnp.where(up, 0.0, (1.0 - 2.0 * ratio) * scale)
        second = (1.0 + ratio) * scale
        return first * density + second * square - scale * cube

    return lax.fori_loop(0, PURIFY, step, initial)


def scaled(gram_stiff, gram_mass):
    n = gram_stiff.shape[0]
    masked = gram_mass * eye(n)
    across = lax.rsqrt(jnp.sum(masked, axis=0, keepdims=True) + 1e-6)
    down = lax.rsqrt(jnp.sum(masked, axis=1, keepdims=True) + 1e-6)
    return across, gram_stiff * down * across, gram_mass * down * across


def ritz_first(gram_stiff, gram_mass):
    gram_stiff = 0.5 * (gram_stiff + gram_stiff.T)
    gram_mass = 0.5 * (gram_mass + gram_mass.T)
    across, stiff, mass = scaled(gram_stiff, gram_mass)
    inverse = inverse_factor(mass, 0)
    reduced = mm_nt(mm(inverse, stiff, HIGHEST), inverse, HIGHEST)
    return inverse * across, 0.5 * (reduced + reduced.T)


def ritz_next(gram_stiff, gram_mass):
    n = gram_stiff.shape[0]
    rest = n - MODES
    across, stiff, mass = scaled(gram_stiff, gram_mass)
    lead = 1.0 + 1e-6
    side = mass[:, :MODES]
    side = jnp.where(sublanes((n, MODES)) < MODES, 0.0, side)
    lower = mass[MODES:, :]
    schur = lower - lead * mm_nt(side[MODES:], side, HIGHEST)
    lane = lanes((rest, n))
    bottom = inverse_factor(jnp.where(lane < MODES, -lead * lower, schur), MODES)
    shape = (MODES, n)
    unit = jnp.where(lanes(shape) == sublanes(shape), 1.0, 0.0)
    inverse = jnp.concatenate([lead**0.5 * unit, bottom], axis=0)
    reduced = mm_nt(mm(inverse, stiff, HIGHEST), inverse, HIGHEST)
    reduced = 0.5 * (reduced + reduced.T)
    rows = purify(reduced)[:MODES]
    change = inverse_factor(mm_nt(rows, rows, HIGHEST), 0)
    rows = mm(change, rows, HIGHEST)
    coefficients = mm(rows, inverse, HIGHEST) * across
    padded = jnp.concatenate([rows, jnp.zeros((rest, n), jnp.float32)], axis=0)
    projected = mm_nt(mm(rows, reduced, HIGHEST), padded, HIGHEST)
    return coefficients, projected


def solve_kernel(
    sizes,
    diag,
    coupling,
    offsets,
    slot_of,
    mass,
    initial,
    mass_out,
    energy_out,
    inverse_diag,
    product,
    ext0,
    ext1,
    ext2,
    ext3,
    stiff_new,
    modes,
    stiff_modes,
    direction,
    stiff_direction,
    edge,
    landing,
    returned,
    part,
    swapped,
    slots,
    summed,
    halo_send,
    halo_recv,
    swap_send,
    swap_recv,
    ring_send,
    ring_recv,
):
    count, blocks = sizes
    ny, nx, cores = TORUS
    side = nx
    me = lax.axis_index("row")
    core = me % cores
    x = (me // cores) % nx
    y = me // (cores * nx)
    partner = me + 1 - 2 * core
    exts = (ext0, ext1, ext2, ext3)

    def peer(phase, k):
        along_x = (1 - core) if phase == 0 else core
        px = (x + k * along_x) % nx
        py = (y + k * (1 - along_x)) % ny
        return (py * nx + px) * cores + core

    def place(phase):
        along_x = (1 - core) if phase == 0 else core
        return x * along_x + y * (1 - along_x)

    barrier = pltpu.get_barrier_semaphore()
    pl.semaphore_signal(barrier, inc=1, device_id={"row": partner}, device_id_type=MESH)
    for phase in range(2):
        for k in range(1, side):
            pl.semaphore_signal(barrier, inc=1, device_id={"row": peer(phase, k)}, device_id_type=MESH)

    for neighbour in ((me + 1) % count, (me + count - 1) % count):
        pl.semaphore_signal(barrier, inc=1, device_id={"row": neighbour}, device_id_type=MESH)

    def forward(app):
        return pltpu.make_async_remote_copy(
            src_ref=exts[app].at[pl.ds(blocks, REACH)],
            dst_ref=landing.at[app],
            send_sem=halo_send.at[app, 0],
            recv_sem=halo_recv.at[app, 0],
            device_id={"row": me + 1},
            device_id_type=MESH,
        )

    def backward(app):
        return pltpu.make_async_remote_copy(
            src_ref=edge.at[app],
            dst_ref=returned.at[app],
            send_sem=halo_send.at[app, 1],
            recv_sem=halo_recv.at[app, 1],
            device_id={"row": me - 1},
            device_id_type=MESH,
        )

    def own_products(ext, b):
        weights = jnp.concatenate([diag[b]] + [coupling[b, s] for s in range(SLOTS)], axis=1)
        out = mm(ext[b + REACH], weights, HIGH)
        stiff_new[b] = out[:, :WIDTH]
        for s in range(SLOTS):
            product[b, s] = out[:, (s + 1) * WIDTH : (s + 2) * WIDTH]

    def gathered_products(ext, b):
        taken = jnp.concatenate(
            [ext[b + REACH - offsets[b, s]] for s in range(SLOTS)], axis=1
        )
        weights = jnp.concatenate([coupling[b, s] for s in range(SLOTS)], axis=1)
        return mm_nt(taken, weights, HIGH)

    def apply_stiffness(app, wait_entry):
        ext = exts[app]
        for b in range(REACH):
            own_products(ext, b)
        for e in range(REACH):
            out = jnp.zeros((MODES, WIDTH), jnp.float32)
            for b in range(e + 1):
                out = out + product[b, slot_of[b, b - e + REACH - 1]]
            edge[app, e] = out
        wait_entry()

        @pl.when(me < count - 1)
        def _():
            forward(app).start()

        @pl.when(me > 0)
        def _():
            backward(app).start()

        @pl.loop(1, blocks // REACH)
        def _(group):
            for k in range(REACH):
                own_products(ext, group * REACH + k)

        def spread(b):
            return product[b + 1, slot_of[b + 1, 0]], product[b + 2, slot_of[b + 2, 1]], product[
                b + 3, slot_of[b + 3, 2]], product[b + 4, slot_of[b + 4, 3]]

        @pl.loop(1, blocks // REACH)
        def _(group):
            for k in range(REACH):
                b = group * REACH + k
                d0, d1, d2, d3 = spread(b)
                stiff_new[b] = stiff_new[b] + gathered_products(ext, b) + ((d0 + d1) + (d2 + d3))

        @pl.when(me > 0)
        def _():
            forward(app).wait_recv()
            ext[0:REACH] = landing[app]

        @pl.when(me == 0)
        def _():
            ext[0:REACH] = jnp.zeros((REACH, MODES, WIDTH), jnp.float32)

        for b in range(REACH):
            d0, d1, d2, d3 = spread(b)
            stiff_new[b] = stiff_new[b] + gathered_products(ext, b) + ((d0 + d1) + (d2 + d3))

        @pl.when(me < count - 1)
        def _():
            backward(app).wait_recv()
            for k in range(REACH):
                b = blocks - REACH + k
                stiff_new[b] = stiff_new[b] + returned[app, k]

        @pl.when(me < count - 1)
        def _():
            forward(app).wait_send()

        @pl.when(me > 0)
        def _():
            backward(app).wait_send()

    def swap(app, stage):
        if stage == 0:
            source, target = part.at[app, 1 - core], swapped.at[app]
        else:
            source, target = summed.at[app, core], summed.at[app, core]
        return pltpu.make_async_remote_copy(
            src_ref=source,
            dst_ref=target,
            send_sem=swap_send.at[app, stage],
            recv_sem=swap_recv.at[app, stage],
            device_id={"row": partner},
            device_id_type=MESH,
        )

    def ring(app, phase, k, slot):
        return pltpu.make_async_remote_copy(
            src_ref=slots.at[app, phase, slot],
            dst_ref=slots.at[app, phase, slot],
            send_sem=ring_send.at[app, phase, k],
            recv_sem=ring_recv.at[app, phase, slot],
            device_id={"row": peer(phase, k)},
            device_id_type=MESH,
        )

    def sum_start(app):
        swap(app, 0).start()

    def sum_finish(app):
        swap(app, 0).wait_recv()
        value = part[app, core] + swapped[app]
        for phase in range(2):
            mine = place(phase)
            slots[app, phase, mine] = value
            for k in range(1, side):
                ring(app, phase, k, mine).start()
            for k in range(1, side):
                ring(app, phase, k, (mine + k) % side).wait_recv()
            value = slots[app, phase, 0]
            for k in range(1, side):
                value = value + slots[app, phase, k]
        summed[app, core] = value
        swap(app, 1).start()
        pltpu.make_async_remote_copy(
            src_ref=summed.at[app, core],
            dst_ref=summed.at[app, 1 - core],
            send_sem=swap_send.at[app, 1],
            recv_sem=swap_recv.at[app, 1],
            device_id={"row": partner},
            device_id_type=MESH,
        ).wait_recv()
        stiff, mass_part = summed[app, 0], summed[app, 1]
        swap(app, 0).wait_send()
        swap(app, 1).wait_send()
        for phase in range(2):
            for k in range(1, side):
                ring(app, phase, k, place(phase)).wait_send()
        return stiff, mass_part

    def wait_barrier():
        pl.semaphore_wait(barrier, 3 + 2 * (side - 1))

    def wide(refs, pieces, group):
        return jnp.concatenate(
            [jnp.concatenate([ref[group * pieces + k + shift] for ref, shift in refs], axis=0)
             for k in range(pieces)], axis=1)

    def mass_wide(pieces, group):
        return jnp.concatenate([mass[pl.ds(group * pieces + k, 1), :] for k in range(pieces)], axis=1)

    def grams(app, basis, stiff_basis):
        ext = exts[app]
        order = MODES * len(basis)
        pieces = 4

        def body(group, carry):
            left = wide([(ext, REACH)], pieces, group)
            return (
                carry[0] + mm_nt(left, wide(stiff_basis, pieces, group), HIGH),
                carry[1] + mm_nt(left * mass_wide(pieces, group), wide(basis, pieces, group), HIGH),
            )

        zero = jnp.zeros((MODES, order), jnp.float32)
        stiff, weighted = lax.fori_loop(0, blocks // pieces, body, (zero, zero))
        part[app] = jnp.zeros((2, MODES, WIDTH), jnp.float32)
        part[app, 0, :, 0:order] = stiff
        part[app, 1, :, 0:order] = weighted

    identity = eye(WIDTH)

    @pl.loop(0, blocks)
    def _(b):
        inverse_diag[pl.ds(b, 1), :] = 1.0 / jnp.sum(diag[b] * identity, axis=0, keepdims=True)

    @pl.loop(0, blocks + REACH)
    def _(b):
        product[b, SLOTS] = jnp.zeros((MODES, WIDTH), jnp.float32)

    for b in range(blocks):
        ext0[b + REACH] = initial[:, b * WIDTH : (b + 1) * WIDTH]
    apply_stiffness(0, wait_barrier)
    grams(0, [(ext0, REACH)], [(stiff_new, 0)])
    sum_start(0)
    gram_stiff, gram_mass = sum_finish(0)
    coefficients, projected = ritz_first(gram_stiff[:, :MODES], gram_mass[:, :MODES])
    lead_stiff = projected
    basis, stiff_basis = [(ext0, REACH)], [(stiff_new, 0)]
    previous = None

    for step in range(1, ITERS + 1):
        ext = exts[step]
        order = coefficients.shape[1]
        shape = (MODES, order)
        later = jnp.where(lanes(shape) < MODES, 0.0, coefficients)
        both = coefficients if previous is None else jnp.concatenate([coefficients, later], axis=0)

        def update(group, pieces, basis=basis, stiff_basis=stiff_basis, both=both, ext=ext,
                   projected=projected):
            new = mm(both, wide(basis, pieces, group), HIGH)
            stiff = mm(both, wide(stiff_basis, pieces, group), HIGH)
            weighted = new[:MODES] * mass_wide(pieces, group)
            scale = jnp.concatenate(
                [inverse_diag[pl.ds(group * pieces + k, 1), :] for k in range(pieces)], axis=1)
            residual = (stiff[:MODES] - mm(projected[:, :MODES], weighted, HIGH)) * scale
            for k in range(pieces):
                b = group * pieces + k
                cut = slice(k * WIDTH, (k + 1) * WIDTH)
                modes[b] = new[:MODES, cut]
                stiff_modes[b] = stiff[:MODES, cut]
                ext[b + REACH] = residual[:, cut]
                if both.shape[0] > MODES:
                    direction[b] = new[MODES:, cut]
                    stiff_direction[b] = stiff[MODES:, cut]

        @pl.loop(0, blocks // 4)
        def _(group):
            update(group, 4)

        apply_stiffness(step, lambda: None)
        basis = [(modes, 0), (ext, REACH)]
        stiff_basis = [(stiff_modes, 0), (stiff_new, 0)]
        if previous is not None:
            basis.append((direction, 0))
            stiff_basis.append((stiff_direction, 0))
        grams(step, basis, stiff_basis)
        sum_start(step)
        n = MODES * len(basis)
        shape = (MODES, n)
        lane = lanes(shape)
        unit = jnp.where(lane == sublanes(shape), 0.5, 0.0)
        if previous is None:
            placed = mm(0.5 * lead_stiff, jnp.where(lane == sublanes(shape), 1.0, 0.0), HIGHEST)
            third = None
        else:
            placed = projected
            if placed.shape[1] < n:
                grown = jnp.where(lane == sublanes(shape), 1.0, 0.0)
                placed = mm(placed[:, :MODES], grown, HIGHEST)
            placed = 0.5 * placed
            zero = jnp.zeros((MODES, order), jnp.float32)
            spread_rows = jnp.concatenate([coefficients, zero, later], axis=0)
            third = [
                mm_nt(mm(later, old, HIGHEST), spread_rows, HIGHEST)
                * jnp.where(lane < 2 * MODES, 1.0, 0.5)
                for old in previous
            ]
        summed_stiff, summed_mass = sum_finish(step)
        half = jnp.where((lane >= MODES) & (lane < 2 * MODES), 0.5, 1.0)
        rows = [[placed, summed_stiff[:, :n] * half], [unit, summed_mass[:, :n] * half]]
        if third is not None:
            rows[0].append(third[0])
            rows[1].append(third[1])
        full = [jnp.concatenate(r, axis=0) for r in rows]
        full = [f + f.T for f in full]
        coefficients, projected = ritz_next(full[0], full[1])
        previous = full

    weight = count * blocks * WIDTH / MODES

    @pl.loop(0, blocks // 4)
    def _(group):
        new = mm(coefficients, wide(basis, 4, group), HIGH)
        stiff = mm(coefficients, wide(stiff_basis, 4, group), HIGH)
        density = weight * jnp.sum(new * new, axis=0, keepdims=True) * mass_wide(4, group)
        energy = weight * jnp.sum(new * stiff, axis=0, keepdims=True)
        for k in range(4):
            cut = slice(k * WIDTH, (k + 1) * WIDTH)
            mass_out[pl.ds(group * 4 + k, 1), :] = density[:, cut]
            energy_out[pl.ds(group * 4 + k, 1), :] = energy[:, cut]


def solution(mesh):
    count = mesh.shape["row"]

    def local(diag_blocks, coupling, offsets, mass, initial_modes):
        blocks = diag_blocks.shape[0]
        apps = ITERS + 1
        side = TORUS[1]
        steps = jnp.arange(1, REACH + 1, dtype=jnp.int32)
        hit = offsets[:, :, None] == steps
        slot_of = jnp.where(hit.any(axis=1), jnp.argmax(hit, axis=1), SLOTS)
        slot_of = jnp.pad(slot_of.astype(jnp.int32), ((0, REACH), (0, 0)), constant_values=SLOTS)
        vector = pltpu.VMEM((blocks, MODES, WIDTH), jnp.float32)
        extended = pltpu.VMEM((blocks + REACH, MODES, WIDTH), jnp.float32)
        halo = pltpu.VMEM((apps, REACH, MODES, WIDTH), jnp.float32)
        outs = pl.pallas_call(
            lambda *refs: solve_kernel((count, blocks), *refs),
            out_shape=[jax.ShapeDtypeStruct((blocks, WIDTH), jnp.float32)] * 2,
            in_specs=[
                pl.BlockSpec(memory_space=pltpu.VMEM),
                pl.BlockSpec(memory_space=pltpu.VMEM),
                pl.BlockSpec(memory_space=pltpu.SMEM),
                pl.BlockSpec(memory_space=pltpu.SMEM),
                pl.BlockSpec(memory_space=pltpu.VMEM),
                pl.BlockSpec(memory_space=pltpu.VMEM),
            ],
            out_specs=[pl.BlockSpec(memory_space=pltpu.VMEM)] * 2,
            scratch_shapes=[
                pltpu.VMEM((blocks, WIDTH), jnp.float32),
                pltpu.VMEM((blocks + REACH, SLOTS + 1, MODES, WIDTH), jnp.float32),
                extended,
                extended,
                extended,
                extended,
                vector,
                vector,
                vector,
                vector,
                vector,
                halo,
                halo,
                halo,
                pltpu.VMEM((apps, 2, MODES, WIDTH), jnp.float32),
                pltpu.VMEM((apps, MODES, WIDTH), jnp.float32),
                pltpu.VMEM((apps, 2, side, MODES, WIDTH), jnp.float32),
                pltpu.VMEM((apps, 2, MODES, WIDTH), jnp.float32),
                pltpu.SemaphoreType.DMA((apps, 2)),
                pltpu.SemaphoreType.DMA((apps, 2)),
                pltpu.SemaphoreType.DMA((apps, 2)),
                pltpu.SemaphoreType.DMA((apps, 2)),
                pltpu.SemaphoreType.DMA((apps, 2, side)),
                pltpu.SemaphoreType.DMA((apps, 2, side)),
            ],
            compiler_params=pltpu.CompilerParams(
                collective_id=0, has_side_effects=True, vmem_limit_bytes=48 << 20
            ),
            name="lobpcg",
        )(
            diag_blocks,
            coupling,
            offsets,
            slot_of,
            mass.reshape(blocks, WIDTH),
            initial_modes,
        )
        return outs[0].reshape(-1), outs[1].reshape(-1)

    spec = ("sub", "row")
    return jax.shard_map(
        local,
        mesh=mesh,
        in_specs=(
            P(spec, None, None),
            P(spec, None, None, None),
            P(spec, None),
            P(spec),
            P(None, spec),
        ),
        out_specs=(P(spec), P(spec)),
        check_vma=False,
    )
```

```python
import jax
import jax.numpy as jnp
from jax import lax
from jax.experimental import pallas as pl
from jax.experimental.pallas import tpu as pltpu
from jax.sharding import PartitionSpec as P

MODES = 32
REACH = 4
SLOTS = 3
ITERS = 3
PURIFY = 28
WIDTH = 128
TORUS = (8, 8, 2)
MESH = pl.DeviceIdType.MESH

HIGH = lax.Precision.HIGH
HIGHEST = lax.Precision.HIGHEST


def mm(a, b, precision):
    return lax.dot_general(
        a, b, (((1,), (0,)), ((), ())), precision=precision, preferred_element_type=jnp.float32
    )


def mm_nt(a, b, precision):
    return lax.dot_general(
        a, b, (((1,), (1,)), ((), ())), precision=precision, preferred_element_type=jnp.float32
    )


def lanes(shape):
    return lax.broadcasted_iota(jnp.int32, shape, 1)


def sublanes(shape):
    return lax.broadcasted_iota(jnp.int32, shape, 0)


def eye(n):
    return (sublanes((n, n)) == lanes((n, n))).astype(jnp.float32)


def total(x):
    return jnp.sum(jnp.sum(x, axis=0, keepdims=True), axis=1, keepdims=True)


def inverse_factor(table, first):
    rows, cols = table.shape
    done = []
    for start in range(0, rows, 8):
        live = table.shape[0]
        column = [
            jnp.broadcast_to(table[:, first + start + k : first + start + k + 1], (live, cols))
            for k in range(8)
        ]
        index = sublanes((live, cols))
        lane = lanes((live, cols))
        for k in range(8):
            at = first + start + k
            pivot = column[k][k : k + 1, :]
            scale = lax.rsqrt(pivot)
            row = jnp.where(lane[0:1] == at, 1.0, table[k : k + 1, :]) * scale
            factor = jnp.where(index > k, column[k] * scale, 0.0)
            table = jnp.where((index > k) & (lane == at), 0.0, table) - factor * row
            table = jnp.where(index == k, row, table)
            for m in range(k + 1, 8):
                column[m] = column[m] - factor * (column[m][k : k + 1, :] * scale)
        done.append(table[:8])
        table = table[8:]
    result = jnp.concatenate(done, axis=0) if len(done) > 1 else done[0]
    shape = (rows, cols)
    return jnp.where(lanes(shape) <= sublanes(shape) + first, result, 0.0)


def purify(matrix):
    n = matrix.shape[0]
    identity = eye(n)
    diagonal = jnp.sum(matrix * identity, axis=0, keepdims=True)
    radius = jnp.sum(jnp.abs(matrix), axis=0, keepdims=True) - jnp.abs(diagonal)
    center = jnp.sum(diagonal, axis=1, keepdims=True) / n
    highest = jnp.max(diagonal + radius, axis=1, keepdims=True)
    lowest = jnp.min(diagonal - radius, axis=1, keepdims=True)
    factor = jnp.minimum(
        MODES / jnp.maximum(highest - center, 1e-6), (n - MODES) / jnp.maximum(center - lowest, 1e-6)
    )
    initial = factor / n * (center * identity - matrix) + MODES / n * identity

    def step(index, density):
        square = mm(density, density, HIGHEST)
        cube = mm(square, density, HIGHEST)
        denominator = total((density - square) * identity)
        numerator = total(square * (identity - density))
        safe = jnp.where(jnp.abs(denominator) > 1e-12, denominator, 1.0)
        ratio = jnp.clip(numerator / safe, 0.0, 1.0)
        up = ratio >= 0.5
        scale = 1.0 / jnp.maximum(jnp.where(up, ratio, 1.0 - ratio), 0.5)
        first = jnp.where(up, 0.0, (1.0 - 2.0 * ratio) * scale)
        second = (1.0 + ratio) * scale
        return first * density + second * square - scale * cube

    return lax.fori_loop(0, PURIFY, step, initial)


def pack(square):
    return jnp.concatenate([square[8 * k : 8 * k + 8] for k in range(4)], axis=1)


def unpack(tile):
    return jnp.concatenate([tile[:, MODES * k : MODES * (k + 1)] for k in range(4)], axis=0)


def scales(gram_mass):
    masked = gram_mass * eye(gram_mass.shape[0])
    across = lax.rsqrt(jnp.sum(masked, axis=0, keepdims=True) + 1e-6)
    down = lax.rsqrt(jnp.sum(masked, axis=1, keepdims=True) + 1e-6)
    return across, gram_mass * down * across


def first_factor(gram_mass):
    across, mass = scales(0.5 * (gram_mass + gram_mass.T))
    return inverse_factor(mass, 0) * across


def next_factor(gram_mass):
    n = gram_mass.shape[0]
    rest = n - MODES
    across, mass = scales(gram_mass)
    lead = 1.0 + 1e-6
    side = mass[:, :MODES]
    side = jnp.where(sublanes((n, MODES)) < MODES, 0.0, side)
    lower = mass[MODES:, :]
    schur = lower - lead * mm_nt(side[MODES:], side, HIGHEST)
    lane = lanes((rest, n))
    bottom = inverse_factor(jnp.where(lane < MODES, -lead * lower, schur), MODES)
    shape = (MODES, n)
    unit = jnp.where(lanes(shape) == sublanes(shape), lead**0.5, 0.0)
    return jnp.concatenate([unit, bottom], axis=0) * across


def ritz_rows(reduced, factor):
    n = reduced.shape[0]
    rows = purify(reduced)[:MODES]
    change = inverse_factor(mm_nt(rows, rows, HIGHEST), 0)
    rows = mm(change, rows, HIGHEST)
    coefficients = mm(rows, factor, HIGHEST)
    padded = jnp.concatenate([rows, jnp.zeros((n - MODES, n), jnp.float32)], axis=0)
    projected = mm_nt(mm(rows, reduced, HIGHEST), padded, HIGHEST)
    return coefficients, projected


def solve_kernel(
    sizes,
    diag_hbm,
    coupling_hbm,
    offsets,
    mass_hbm,
    initial_hbm,
    mass_out,
    energy_out,
    diag,
    coupling,
    mass,
    slot_of,
    inverse_diag,
    product,
    ext0,
    ext1,
    ext2,
    ext3,
    stiff_new,
    modes,
    stiff_modes,
    direction,
    stiff_direction,
    edge,
    landing,
    returned,
    part,
    swapped,
    slots,
    summed,
    late_part,
    late_first,
    late_second,
    load_sem,
    matrix_sem,
    halo_send,
    halo_recv,
    swap_send,
    swap_recv,
    ring_send,
    ring_recv,
    late_send,
    late_recv_first,
    late_recv_second,
):
    count, blocks = sizes
    ny, nx, cores = TORUS
    side = nx
    me = lax.axis_index("row")
    core = me % cores
    x = (me // cores) % nx
    y = me // (cores * nx)
    partner = me + 1 - 2 * core
    exts = (ext0, ext1, ext2, ext3)
    groups = blocks // REACH

    def device(px, py, pcore):
        return {"row": (py * nx + px) * cores + pcore}

    def peer(phase, k, pcore):
        along_x = (1 - core) if phase == 0 else core
        return device((x + k * along_x) % nx, (y + k * (1 - along_x)) % ny, pcore)

    def place(phase):
        along_x = (1 - core) if phase == 0 else core
        return x * along_x + y * (1 - along_x)

    barrier = pltpu.get_barrier_semaphore()
    greeted = [{"row": partner}, {"row": (me + 1) % count}, {"row": (me + count - 1) % count}]
    for k in range(1, side):
        for pcore in range(cores):
            greeted += [device((x + k) % nx, y, pcore), device(x, (y + k) % ny, pcore)]
    for other in greeted:
        pl.semaphore_signal(barrier, inc=1, device_id=other, device_id_type=MESH)

    loads = [
        pltpu.make_async_copy(
            initial_hbm.at[:, pl.ds(b * WIDTH, WIDTH)], ext0.at[b + REACH], load_sem.at[b]
        )
        for b in range(blocks)
    ]
    loads.append(pltpu.make_async_copy(mass_hbm, mass, load_sem.at[blocks]))
    matrix_loads = [
        [
            pltpu.make_async_copy(
                ref.at[pl.ds(g * REACH, REACH)], out.at[pl.ds(g * REACH, REACH)], matrix_sem.at[i, g]
            )
            for i, (ref, out) in enumerate([(diag_hbm, diag), (coupling_hbm, coupling)])
        ]
        for g in range(groups)
    ]
    for copy in loads:
        copy.start()
    for pair in matrix_loads:
        for copy in pair:
            copy.start()

    def send(source, target, send_sem, recv_sem, other):
        return pltpu.make_async_remote_copy(
            src_ref=source,
            dst_ref=target,
            send_sem=send_sem,
            recv_sem=recv_sem,
            device_id=other,
            device_id_type=MESH,
        )

    def forward(app):
        return send(
            exts[app].at[pl.ds(blocks, REACH)],
            landing.at[app],
            halo_send.at[app, 0],
            halo_recv.at[app, 0],
            {"row": me + 1},
        )

    def backward(app):
        return send(
            edge.at[app],
            returned.at[app],
            halo_send.at[app, 1],
            halo_recv.at[app, 1],
            {"row": me - 1},
        )

    def own_products(ext, b):
        weights = jnp.concatenate([diag[b]] + [coupling[b, s] for s in range(SLOTS)], axis=1)
        out = mm(ext[b + REACH], weights, HIGH)
        stiff_new[b] = out[:, :WIDTH]
        for s in range(SLOTS):
            product[b, s] = out[:, (s + 1) * WIDTH : (s + 2) * WIDTH]

    def other_products(ext, b):
        taken = jnp.concatenate([ext[b + REACH - offsets[b, s]] for s in range(SLOTS)], axis=1)
        weights = jnp.concatenate([coupling[b, s] for s in range(SLOTS)], axis=1)
        spread = [product[b + d, slot_of[b + d, d - 1]] for d in range(1, REACH + 1)]
        spread = (spread[0] + spread[1]) + (spread[2] + spread[3])
        stiff_new[b] = stiff_new[b] + mm_nt(taken, weights, HIGH) + spread

    def apply_stiffness(app, ready, hooks):
        ext = exts[app]
        ready(0)
        for b in range(REACH):
            own_products(ext, b)
        for e in range(REACH):
            out = jnp.zeros((MODES, WIDTH), jnp.float32)
            for b in range(e + 1):
                out = out + product[b, slot_of[b, b - e + REACH - 1]]
            edge[app, e] = out
        hooks[0]()

        @pl.when(me < count - 1)
        def _():
            forward(app).start()

        @pl.when(me > 0)
        def _():
            backward(app).start()

        for g in range(1, groups):
            ready(g)
            for b in range(g * REACH, (g + 1) * REACH):
                own_products(ext, b)
        hooks[1]()
        for b in range(REACH, blocks):
            other_products(ext, b)
        hooks[2]()

        @pl.when(me > 0)
        def _():
            forward(app).wait_recv()
            ext[0:REACH] = landing[app]

        @pl.when(me == 0)
        def _():
            ext[0:REACH] = jnp.zeros((REACH, MODES, WIDTH), jnp.float32)

        for b in range(REACH):
            other_products(ext, b)

        @pl.when(me < count - 1)
        def _():
            backward(app).wait_recv()
            for k in range(REACH):
                b = blocks - REACH + k
                stiff_new[b] = stiff_new[b] + returned[app, k]

    def swap(app, stage):
        if stage == 0:
            source, target = part.at[app, 1 - core], swapped.at[app]
        else:
            source, target = summed.at[app, core], summed.at[app, core]
        return send(
            source, target, swap_send.at[app, stage], swap_recv.at[app, stage], {"row": partner}
        )

    def ring(app, phase, k, slot):
        return send(
            slots.at[app, phase, slot],
            slots.at[app, phase, slot],
            ring_send.at[app, phase, k],
            ring_recv.at[app, phase, slot],
            peer(phase, k, core),
        )

    def ring_start(app, phase, value):
        mine = place(phase)
        slots[app, phase, mine] = value
        for k in range(1, side):
            ring(app, phase, k, mine).start()

    def ring_finish(app, phase):
        mine = place(phase)
        for k in range(1, side):
            ring(app, phase, k, (mine + k) % side).wait_recv()
        value = slots[app, phase, 0]
        for k in range(1, side):
            value = value + slots[app, phase, k]
        return value

    def early_first(app):
        swap(app, 0).wait_recv()
        ring_start(app, 0, part[app, core] + swapped[app])

    def early_second(app):
        ring_start(app, 1, ring_finish(app, 0))

    def early_third(app):
        summed[app, core] = ring_finish(app, 1)
        swap(app, 1).start()

    def early_last(app):
        send(
            summed.at[app, core],
            summed.at[app, 1 - core],
            swap_send.at[app, 1],
            swap_recv.at[app, 1],
            {"row": partner},
        ).wait_recv()
        return summed[app, 0], summed[app, 1]

    def late_first_send(app, half, k):
        along_x = 1 - half
        target = device((x + k * along_x) % nx, (y + k * half) % ny, half)
        slot = (x * along_x + y * half) * cores + core
        return send(
            late_part.at[app, half],
            late_first.at[app, slot],
            late_send.at[app, 0, half, k],
            late_recv_first.at[app, slot],
            target,
        )

    def late_first_partner(app):
        half = 1 - core
        slot = (x * core + y * half) * cores + core
        return send(
            late_part.at[app, half],
            late_first.at[app, slot],
            late_send.at[app, 0, half, 0],
            late_recv_first.at[app, slot],
            {"row": partner},
        )

    def late_second_send(app, pcore, k):
        where = place(1)
        return send(
            late_second.at[app, core, where],
            late_second.at[app, core, where],
            late_send.at[app, 1, pcore, k],
            late_recv_second.at[app, core, where],
            peer(1, k, pcore),
        )

    def late_second_partner(app):
        where = place(1)
        return send(
            late_second.at[app, core, where],
            late_second.at[app, core, where],
            late_send.at[app, 1, 1 - core, 0],
            late_recv_second.at[app, core, where],
            {"row": partner},
        )

    def late_start(app, block):
        tile = pack(block)
        late_part[app, 0] = tile[0:4]
        late_part[app, 1] = tile[4:8]
        late_first[app, place(0) * cores + core] = late_part[app, core]
        for k in range(1, side):
            for half in range(2):
                late_first_send(app, half, k).start()
        late_first_partner(app).start()

    def arrived(buffer, sem, index):
        return send(
            buffer.at[index], buffer.at[index], late_send.at[0, 0, 0, 0], sem.at[index], {"row": partner}
        ).wait_recv()

    def late_middle(app):
        mine = place(0) * cores + core
        for k in range(1, side * cores):
            arrived(late_first, late_recv_first, (app, (mine + k) % (side * cores)))
        value = late_first[app, 0]
        for k in range(1, side * cores):
            value = value + late_first[app, k]
        late_second[app, core, place(1)] = value
        for k in range(1, side):
            for pcore in range(cores):
                late_second_send(app, pcore, k).start()
        late_second_partner(app).start()

    def late_finish(app):
        for k in range(1, side):
            arrived(late_second, late_recv_second, (app, core, (place(1) + k) % side))
        for k in range(side):
            arrived(late_second, late_recv_second, (app, 1 - core, k))
        halves = []
        for half in range(2):
            value = late_second[app, half, 0]
            for k in range(1, side):
                value = value + late_second[app, half, k]
            halves.append(value)
        return unpack(jnp.concatenate(halves, axis=0))

    def drain(app):
        @pl.when(me < count - 1)
        def _():
            forward(app).wait_send()

        @pl.when(me > 0)
        def _():
            backward(app).wait_send()

        for stage in range(2):
            swap(app, stage).wait_send()
        for phase in range(2):
            for k in range(1, side):
                ring(app, phase, k, place(phase)).wait_send()
        for k in range(1, side):
            for half in range(2):
                late_first_send(app, half, k).wait_send()
                late_second_send(app, half, k).wait_send()
        late_first_partner(app).wait_send()
        late_second_partner(app).wait_send()

    def wide(refs, group):
        return jnp.concatenate(
            [
                jnp.concatenate([ref[group * REACH + k + shift] for ref, shift in refs], axis=0)
                for k in range(REACH)
            ],
            axis=1,
        )

    def wide_row(ref, group):
        return jnp.concatenate(
            [ref[group * REACH + k : group * REACH + k + 1, :] for k in range(REACH)], axis=1
        )

    def late_block(app):
        ext = exts[app]
        acc = mm_nt(wide([(ext, REACH)], 0), wide([(stiff_new, 0)], 0), HIGH)
        for g in range(1, groups):
            acc = acc + mm_nt(wide([(ext, REACH)], g), wide([(stiff_new, 0)], g), HIGH)
        return acc

    for b in range(blocks):
        for d in range(1, REACH + 1):
            slot = SLOTS
            for s in range(SLOTS):
                slot = jnp.where(offsets[b, s] == d, s, slot)
            slot_of[b, d - 1] = slot
    for b in range(blocks, blocks + REACH):
        for d in range(REACH):
            slot_of[b, d] = SLOTS
    for b in range(blocks + REACH):
        product[b, SLOTS] = jnp.zeros((MODES, WIDTH), jnp.float32)
    part[...] = jnp.zeros(part.shape, jnp.float32)
    for copy in loads:
        copy.wait()
    acc = jnp.zeros((MODES, MODES), jnp.float32)
    for g in range(groups):
        left = wide([(ext0, REACH)], g)
        acc = acc + mm_nt(left * wide_row(mass, g), left, HIGH)
    part[0, 1, :, 0:MODES] = acc

    def ready(g):
        for copy in matrix_loads[g]:
            copy.wait()

    def enter():
        pl.semaphore_wait(barrier, len(greeted))
        swap(0, 0).start()

    apply_stiffness(0, ready, (enter, lambda: early_first(0), lambda: early_second(0)))
    late_start(0, late_block(0))
    identity = eye(WIDTH)
    for b in range(blocks):
        inverse_diag[b : b + 1, :] = 1.0 / jnp.sum(diag[b] * identity, axis=0, keepdims=True)
    late_middle(0)
    early_third(0)
    _, gram_mass = early_last(0)
    factor = first_factor(gram_mass[:, :MODES])
    block = late_finish(0)
    projected = mm_nt(mm(factor, block, HIGHEST), factor, HIGHEST)
    projected = 0.5 * (projected + projected.T)
    coefficients = factor
    basis, stiff_basis = [(ext0, REACH)], [(stiff_new, 0)]
    previous = None

    for step in range(1, ITERS + 1):
        ext = exts[step]
        order = coefficients.shape[1]
        later = jnp.where(lanes((MODES, order)) < MODES, 0.0, coefficients)
        moving = previous is not None
        both = jnp.concatenate([coefficients, later], axis=0) if moving else coefficients
        n = MODES * (3 if moving else 2)
        stiff_acc = jnp.zeros((MODES, n), jnp.float32)
        mass_acc = jnp.zeros((MODES, n), jnp.float32)
        for g in range(groups):
            new = mm(both, wide(basis, g), HIGH)
            stiff = mm(both, wide(stiff_basis, g), HIGH)
            masses = wide_row(mass, g)
            residual = stiff[:MODES] - mm(projected[:, :MODES], new[:MODES] * masses, HIGH)
            residual = residual * wide_row(inverse_diag, g)
            for k in range(REACH):
                b = g * REACH + k
                cut = slice(k * WIDTH, (k + 1) * WIDTH)
                modes[b] = new[:MODES, cut]
                stiff_modes[b] = stiff[:MODES, cut]
                ext[b + REACH] = residual[:, cut]
                if moving:
                    direction[b] = new[MODES:, cut]
                    stiff_direction[b] = stiff[MODES:, cut]
            zero = jnp.zeros(residual.shape, jnp.float32)
            right = [new[:MODES], residual] + ([new[MODES:]] if moving else [])
            stiff_right = [stiff[:MODES], zero] + ([stiff[MODES:]] if moving else [])
            mass_acc = mass_acc + mm_nt(residual * masses, jnp.concatenate(right, axis=0), HIGH)
            stiff_acc = stiff_acc + mm_nt(residual, jnp.concatenate(stiff_right, axis=0), HIGH)
        part[step, 0, :, 0:n] = stiff_acc
        part[step, 1, :, 0:n] = mass_acc
        apply_stiffness(
            step,
            lambda g: None,
            (
                lambda: swap(step, 0).start(),
                lambda: early_first(step),
                lambda: early_second(step),
            ),
        )
        basis = [(modes, 0), (ext, REACH)] + ([(direction, 0)] if moving else [])
        stiff_basis = [(stiff_modes, 0), (stiff_new, 0)] + ([(stiff_direction, 0)] if moving else [])
        late_start(step, late_block(step))
        shape = (MODES, n)
        lane = lanes(shape)
        unit = jnp.where(lane == sublanes(shape), 1.0, 0.0)
        placed = mm(0.5 * projected[:, :MODES], unit, HIGHEST)
        third = []
        if moving:
            zero = jnp.zeros((MODES, order), jnp.float32)
            spread_rows = jnp.concatenate([coefficients, zero, later], axis=0)
            third = [
                [
                    mm_nt(mm(later, old, HIGHEST), spread_rows, HIGHEST)
                    * jnp.where(lane < 2 * MODES, 1.0, 0.5)
                ]
                for old in previous
            ]
        else:
            third = [[], []]
        late_middle(step)
        early_third(step)
        drain(step - 1)
        early_stiff, early_mass = early_last(step)
        half = jnp.where((lane >= MODES) & (lane < 2 * MODES), 0.5, 1.0)
        rest = jnp.concatenate([placed, early_stiff[:, :n]] + third[0], axis=0)
        gram_mass = jnp.concatenate([0.5 * unit, early_mass[:, :n] * half] + third[1], axis=0)
        rest = rest + rest.T
        gram_mass = gram_mass + gram_mass.T
        factor = next_factor(gram_mass)
        known = mm_nt(mm(factor, rest, HIGHEST), factor, HIGHEST)
        middle = factor[:, MODES : 2 * MODES]
        block = late_finish(step)
        reduced = known + mm_nt(mm(middle, block, HIGHEST), middle, HIGHEST)
        reduced = 0.5 * (reduced + reduced.T)
        coefficients, projected = ritz_rows(reduced, factor)
        if step < ITERS:
            spot = jnp.where(lane == sublanes(shape) + MODES, 1.0, 0.0)
            inner = [jnp.zeros(shape, jnp.float32), mm(block, spot, HIGHEST)]
            inner += [jnp.zeros(shape, jnp.float32)] * (n // MODES - 2)
            previous = [rest + jnp.concatenate(inner, axis=0), gram_mass]

    for g in range(groups):
        new = mm(coefficients, wide(basis, g), HIGH)
        stiff = mm(coefficients, wide(stiff_basis, g), HIGH)
        density = jnp.sum(new * new, axis=0, keepdims=True)
        energy = jnp.sum(new * stiff, axis=0, keepdims=True)
        for k in range(REACH):
            cut = slice(k * WIDTH, (k + 1) * WIDTH)
            mass_out[g * REACH + k : g * REACH + k + 1, :] = density[:, cut]
            energy_out[g * REACH + k : g * REACH + k + 1, :] = energy[:, cut]
    drain(ITERS)


def solution(mesh):
    count = mesh.shape["row"]

    def local(diag_blocks, coupling, offsets, mass, initial_modes):
        blocks = diag_blocks.shape[0]
        apps = ITERS + 1
        side = TORUS[1]
        cores = TORUS[2]
        f32 = jnp.float32
        dma = pltpu.SemaphoreType.DMA
        vector = pltpu.VMEM((blocks, MODES, WIDTH), f32)
        extended = pltpu.VMEM((blocks + REACH, MODES, WIDTH), f32)
        halo = pltpu.VMEM((apps, REACH, MODES, WIDTH), f32)
        squares, energies = pl.pallas_call(
            lambda *refs: solve_kernel((count, blocks), *refs),
            out_shape=[jax.ShapeDtypeStruct((blocks, WIDTH), f32)] * 2,
            in_specs=[
                pl.BlockSpec(memory_space=pl.ANY),
                pl.BlockSpec(memory_space=pl.ANY),
                pl.BlockSpec(memory_space=pltpu.SMEM),
                pl.BlockSpec(memory_space=pl.ANY),
                pl.BlockSpec(memory_space=pl.ANY),
            ],
            out_specs=[pl.BlockSpec(memory_space=pltpu.VMEM)] * 2,
            scratch_shapes=[
                pltpu.VMEM((blocks, WIDTH, WIDTH), f32),
                pltpu.VMEM((blocks, SLOTS, WIDTH, WIDTH), f32),
                pltpu.VMEM((blocks, WIDTH), f32),
                pltpu.SMEM((blocks + REACH, REACH), jnp.int32),
                pltpu.VMEM((blocks, WIDTH), f32),
                pltpu.VMEM((blocks + REACH, SLOTS + 1, MODES, WIDTH), f32),
                extended,
                extended,
                extended,
                extended,
                vector,
                vector,
                vector,
                vector,
                vector,
                halo,
                halo,
                halo,
                pltpu.VMEM((apps, 2, MODES, WIDTH), f32),
                pltpu.VMEM((apps, MODES, WIDTH), f32),
                pltpu.VMEM((apps, 2, side, MODES, WIDTH), f32),
                pltpu.VMEM((apps, 2, MODES, WIDTH), f32),
                pltpu.VMEM((apps, 2, 4, WIDTH), f32),
                pltpu.VMEM((apps, side * cores, 4, WIDTH), f32),
                pltpu.VMEM((apps, 2, side, 4, WIDTH), f32),
                dma((blocks + 1,)),
                dma((2, blocks // REACH)),
                dma((apps, 2)),
                dma((apps, 2)),
                dma((apps, 2)),
                dma((apps, 2)),
                dma((apps, 2, side)),
                dma((apps, 2, side)),
                dma((apps, 2, 2, side)),
                dma((apps, side * cores)),
                dma((apps, 2, side)),
            ],
            compiler_params=pltpu.CompilerParams(
                collective_id=0, has_side_effects=True, vmem_limit_bytes=60 << 20
            ),
            name="lobpcg",
        )(diag_blocks, coupling, offsets, mass.reshape(blocks, WIDTH), initial_modes)
        weight = count * blocks * WIDTH / MODES
        return weight * mass * squares.reshape(-1), weight * energies.reshape(-1)

    spec = ("sub", "row")
    return jax.shard_map(
        local,
        mesh=mesh,
        in_specs=(
            P(spec, None, None),
            P(spec, None, None, None),
            P(spec, None),
            P(spec),
            P(None, spec),
        ),
        out_specs=(P(spec), P(spec)),
        check_vma=False,
    )
```

```python
import jax
import jax.numpy as jnp
from jax import lax
from jax.experimental import pallas as pl
from jax.experimental.pallas import tpu as pltpu
from jax.sharding import PartitionSpec as P

MODES = 32
REACH = 4
SLOTS = 3
ITERS = 3
PURIFY = 28
WIDTH = 128
TORUS = (8, 8, 2)
MESH = pl.DeviceIdType.MESH
CHANNELS = ((1, 1), (2, 1, 1), (3, 2, 1), (3, 2, 1))

HIGHEST = lax.Precision.HIGHEST


def mm(a, b, precision):
    return lax.dot_general(
        a, b, (((1,), (0,)), ((), ())), precision=precision, preferred_element_type=jnp.float32
    )


def mm_nt(a, b, precision):
    return lax.dot_general(
        a, b, (((1,), (1,)), ((), ())), precision=precision, preferred_element_type=jnp.float32
    )


def split(value):
    high = value.astype(jnp.bfloat16)
    return high, (value - high.astype(jnp.float32)).astype(jnp.bfloat16)


def mm3(a, b, transposed=False):
    contract = (((1,), (1 if transposed else 0,)), ((), ()))
    a_high, a_low = split(a)
    b_high, b_low = b if isinstance(b, tuple) else split(b)
    rows = a.shape[0]
    top = lax.dot_general(
        jnp.concatenate([a_high, a_low], axis=0),
        b_high,
        contract,
        preferred_element_type=jnp.float32,
    )
    rest = lax.dot_general(a_high, b_low, contract, preferred_element_type=jnp.float32)
    return (top[:rows] + rest) + top[rows:]


def lanes(shape):
    return lax.broadcasted_iota(jnp.int32, shape, 1)


def sublanes(shape):
    return lax.broadcasted_iota(jnp.int32, shape, 0)


def eye(n):
    return (sublanes((n, n)) == lanes((n, n))).astype(jnp.float32)


def total(x):
    return jnp.sum(jnp.sum(x, axis=0, keepdims=True), axis=1, keepdims=True)


def inverse_factor(table, first):
    rows, cols = table.shape
    done = []
    for start in range(0, rows, 8):
        live = table.shape[0]
        column = [
            jnp.broadcast_to(table[:, first + start + k : first + start + k + 1], (live, cols))
            for k in range(8)
        ]
        index = sublanes((live, cols))
        lane = lanes((live, cols))
        for k in range(8):
            at = first + start + k
            pivot = column[k][k : k + 1, :]
            scale = lax.rsqrt(pivot)
            row = jnp.where(lane[0:1] == at, 1.0, table[k : k + 1, :]) * scale
            factor = jnp.where(index > k, column[k] * scale, 0.0)
            table = jnp.where((index > k) & (lane == at), 0.0, table) - factor * row
            table = jnp.where(index == k, row, table)
            for m in range(k + 1, 8):
                column[m] = column[m] - factor * (column[m][k : k + 1, :] * scale)
        done.append(table[:8])
        table = table[8:]
    result = jnp.concatenate(done, axis=0) if len(done) > 1 else done[0]
    shape = (rows, cols)
    return jnp.where(lanes(shape) <= sublanes(shape) + first, result, 0.0)


def purify(matrix):
    n = matrix.shape[0]
    identity = eye(n)
    diagonal = jnp.sum(matrix * identity, axis=0, keepdims=True)
    radius = jnp.sum(jnp.abs(matrix), axis=0, keepdims=True) - jnp.abs(diagonal)
    center = jnp.sum(diagonal, axis=1, keepdims=True) / n
    highest = jnp.max(diagonal + radius, axis=1, keepdims=True)
    lowest = jnp.min(diagonal - radius, axis=1, keepdims=True)
    factor = jnp.minimum(
        MODES / jnp.maximum(highest - center, 1e-6), (n - MODES) / jnp.maximum(center - lowest, 1e-6)
    )
    initial = factor / n * (center * identity - matrix) + MODES / n * identity

    def step(index, density):
        square = mm(density, density, HIGHEST)
        cube = mm(square, density, HIGHEST)
        denominator = total((density - square) * identity)
        numerator = total(square * (identity - density))
        safe = jnp.where(jnp.abs(denominator) > 1e-12, denominator, 1.0)
        ratio = jnp.clip(numerator / safe, 0.0, 1.0)
        up = ratio >= 0.5
        scale = 1.0 / jnp.maximum(jnp.where(up, ratio, 1.0 - ratio), 0.5)
        first = jnp.where(up, 0.0, (1.0 - 2.0 * ratio) * scale)
        second = (1.0 + ratio) * scale
        return first * density + second * square - scale * cube

    return lax.fori_loop(0, PURIFY, step, initial)


def pack32(block):
    return jnp.concatenate([block[8 * k : 8 * k + 8] for k in range(4)], axis=1)


def unpack32(tile):
    return jnp.concatenate([tile[:, MODES * k : MODES * (k + 1)] for k in range(4)], axis=0)


def pack64(block):
    return jnp.concatenate([block[:16], block[16:]], axis=1)


def unpack64(tile):
    return jnp.concatenate([tile[:, : 2 * MODES], tile[:, 2 * MODES :]], axis=0)


def pack96(block):
    last = [block[24:, MODES * k : MODES * (k + 1)] for k in range(3)]
    return jnp.concatenate([block[:24], jnp.concatenate(last, axis=0)], axis=1)


def unpack96(tile):
    last = [tile[8 * k : 8 * k + 8, 3 * MODES :] for k in range(3)]
    return jnp.concatenate([tile[:, : 3 * MODES], jnp.concatenate(last, axis=1)], axis=0)


def scales(gram_mass):
    masked = gram_mass * eye(gram_mass.shape[0])
    across = lax.rsqrt(jnp.sum(masked, axis=0, keepdims=True) + 1e-6)
    down = lax.rsqrt(jnp.sum(masked, axis=1, keepdims=True) + 1e-6)
    return across, gram_mass * down * across


def first_factor(gram_mass):
    across, mass = scales(0.5 * (gram_mass + gram_mass.T))
    return inverse_factor(mass, 0) * across


def next_factor(gram_mass):
    n = gram_mass.shape[0]
    rest = n - MODES
    across, mass = scales(gram_mass)
    lead = 1.0 + 1e-6
    side = mass[:, :MODES]
    side = jnp.where(sublanes((n, MODES)) < MODES, 0.0, side)
    lower = mass[MODES:, :]
    schur = lower - lead * mm_nt(side[MODES:], side, HIGHEST)
    lane = lanes((rest, n))
    bottom = inverse_factor(jnp.where(lane < MODES, -lead * lower, schur), MODES)
    shape = (MODES, n)
    unit = jnp.where(lanes(shape) == sublanes(shape), lead**0.5, 0.0)
    return jnp.concatenate([unit, bottom], axis=0) * across


def ritz_rows(reduced, factor):
    n = reduced.shape[0]
    rows = purify(reduced)[:MODES]
    change = inverse_factor(mm_nt(rows, rows, HIGHEST), 0)
    rows = mm(change, rows, HIGHEST)
    coefficients = mm(rows, factor, HIGHEST)
    padded = jnp.concatenate([rows, jnp.zeros((n - MODES, n), jnp.float32)], axis=0)
    projected = mm_nt(mm(rows, reduced, HIGHEST), padded, HIGHEST)
    return coefficients, projected


def solve_kernel(
    sizes,
    diag_hbm,
    coupling_hbm,
    offsets_hbm,
    mass_hbm,
    initial_hbm,
    mass_out,
    energy_out,
    diag,
    coupling,
    high,
    low,
    mass,
    offsets,
    slot_of,
    inverse_diag,
    product,
    ext0,
    ext1,
    ext2,
    ext3,
    stiff_new,
    modes,
    stiff_modes,
    direction,
    stiff_direction,
    edge,
    landing,
    returned,
    load_sem,
    matrix_sem,
    halo_send,
    halo_recv,
    *channel_refs,
):
    count, blocks = sizes
    ny, nx, cores = TORUS
    side = nx
    me = lax.axis_index("row")
    core = lax.rem(me, cores)
    x = lax.rem(lax.div(me, cores), nx)
    y = lax.div(me, cores * nx)
    partner = me + 1 - 2 * core
    exts = (ext0, ext1, ext2, ext3)
    groups = blocks // REACH

    table_load = pltpu.make_async_copy(offsets_hbm, offsets, load_sem.at[blocks + 1])
    loads = [pltpu.make_async_copy(mass_hbm, mass, load_sem.at[blocks])]
    loads += [
        pltpu.make_async_copy(
            initial_hbm.at[:, pl.ds(b * WIDTH, WIDTH)], ext0.at[b + REACH], load_sem.at[b]
        )
        for b in range(blocks)
    ]
    matrix_loads = [
        [
            pltpu.make_async_copy(
                ref.at[pl.ds(g * REACH, REACH)], out.at[pl.ds(g * REACH, REACH)], matrix_sem.at[i, g]
            )
            for i, (ref, out) in enumerate([(diag_hbm, diag), (coupling_hbm, coupling)])
        ]
        for g in range(groups)
    ]
    table_load.start()
    for copy in loads:
        copy.start()
    for pair in matrix_loads:
        for copy in pair:
            copy.start()

    x_at = [lax.rem(x + k, nx) for k in range(side)]
    y_at = [lax.rem(y + k, ny) for k in range(side)]

    def device(px, py, pcore):
        return {"row": (py * nx + px) * cores + pcore}

    barrier = pltpu.get_barrier_semaphore()
    greeted = [{"row": partner}, {"row": lax.rem(me + 1, count)}, {"row": lax.rem(me + count - 1, count)}]
    for k in range(1, side):
        for pcore in range(cores):
            greeted += [device(x_at[k], y, pcore), device(x, y_at[k], pcore)]
    for other in greeted:
        pl.semaphore_signal(barrier, inc=1, device_id=other, device_id_type=MESH)

    def send(source, target, send_sem, recv_sem, other):
        return pltpu.make_async_remote_copy(
            src_ref=source,
            dst_ref=target,
            send_sem=send_sem,
            recv_sem=recv_sem,
            device_id=other,
            device_id_type=MESH,
        )

    def forward(app):
        return send(
            exts[app].at[pl.ds(blocks, REACH)],
            landing.at[app],
            halo_send.at[app, 0],
            halo_recv.at[app, 0],
            {"row": me + 1},
        )

    def backward(app):
        return send(
            edge.at[app],
            returned.at[app],
            halo_send.at[app, 1],
            halo_recv.at[app, 1],
            {"row": me - 1},
        )

    def own_products(ext, b):
        out = mm3(ext[b + REACH], (high[b], low[b]))
        stiff_new[b] = out[:, :WIDTH]
        for s in range(SLOTS):
            product[b, s] = out[:, (s + 1) * WIDTH : (s + 2) * WIDTH]

    def other_products(ext, b):
        taken = jnp.concatenate([ext[b + REACH - offsets[b, s]] for s in range(SLOTS)], axis=1)
        spread = [product[b + d, slot_of[b + d, d - 1]] for d in range(1, REACH + 1)]
        spread = (spread[0] + spread[1]) + (spread[2] + spread[3])
        out = mm3(taken, (high[b, :, WIDTH:], low[b, :, WIDTH:]), True)
        stiff_new[b] = stiff_new[b] + out + spread

    def apply_stiffness(app, ready, hooks):
        ext = exts[app]
        ready(0)
        for b in range(REACH):
            own_products(ext, b)
        for e in range(REACH):
            out = jnp.zeros((MODES, WIDTH), jnp.float32)
            for b in range(e + 1):
                out = out + product[b, slot_of[b, b - e + REACH - 1]]
            edge[app, e] = out
        hooks[0]()

        @pl.when(me < count - 1)
        def _():
            forward(app).start()

        @pl.when(me > 0)
        def _():
            backward(app).start()

        for g in range(1, groups):
            ready(g)
            for b in range(g * REACH, (g + 1) * REACH):
                own_products(ext, b)
        hooks[1]()
        for b in range(REACH, blocks):
            other_products(ext, b)

        @pl.when(me > 0)
        def _():
            forward(app).wait_recv()
            ext[0:REACH] = landing[app]

        @pl.when(me == 0)
        def _():
            ext[0:REACH] = jnp.zeros((REACH, MODES, WIDTH), jnp.float32)

        for b in range(REACH):
            other_products(ext, b)

        @pl.when(me < count - 1)
        def _():
            backward(app).wait_recv()
            for k in range(REACH):
                b = blocks - REACH + k
                stiff_new[b] = stiff_new[b] + returned[app, k]

    class Channel:
        def __init__(self, refs):
            (self.part, self.first, self.second, self.sends, self.first_sem, self.second_sem) = refs
            self.own_first = (x * (1 - core) + y * core) * cores + core
            self.own_second = y * (1 - core) + x * core

        def first_send(self, half, k):
            if half == 0:
                slot, target = x * cores + core, device(x_at[k], y, 0)
            else:
                slot, target = y * cores + core, device(x, y_at[k], 1)
            return send(
                self.part.at[half],
                self.first.at[slot],
                self.sends.at[0, half, k],
                self.first_sem.at[slot],
                target,
            )

        def first_partner(self):
            half = 1 - core
            slot = (x * core + y * half) * cores + core
            return send(
                self.part.at[half],
                self.first.at[slot],
                self.sends.at[0, half, 0],
                self.first_sem.at[slot],
                {"row": partner},
            )

        def second_send(self, pcore, k):
            where = self.own_second
            px = x * (1 - core) + x_at[k] * core
            py = y_at[k] * (1 - core) + y * core
            return send(
                self.second.at[core, where],
                self.second.at[core, where],
                self.sends.at[1, pcore, k],
                self.second_sem.at[core, where],
                device(px, py, pcore),
            )

        def second_partner(self):
            where = self.own_second
            return send(
                self.second.at[core, where],
                self.second.at[core, where],
                self.sends.at[1, 1 - core, 0],
                self.second_sem.at[core, where],
                {"row": partner},
            )

        def arrived(self, buffer, sem, index):
            send(
                buffer.at[index], buffer.at[index], self.sends.at[0, 0, 0], sem.at[index],
                {"row": partner},
            ).wait_recv()

        def store(self, packed):
            rows = packed.shape[0] // 2
            self.part[0] = packed[:rows]
            self.part[1] = packed[rows:]

        def start(self):
            self.first[self.own_first] = self.part[core]
            for k in range(1, side):
                for half in range(2):
                    self.first_send(half, k).start()
            self.first_partner().start()

        def middle(self):
            slots = side * cores
            for k in range(1, slots):
                self.arrived(self.first, self.first_sem, lax.rem(self.own_first + k, slots))
            values = [self.first[k] for k in range(slots)]
            while len(values) > 1:
                values = [p + q for p, q in zip(values[::2], values[1::2])]
            self.second[core, self.own_second] = values[0]
            for k in range(1, side):
                for pcore in range(cores):
                    self.second_send(pcore, k).start()
            self.second_partner().start()

        def finish(self):
            for k in range(1, side):
                self.arrived(
                    self.second, self.second_sem, (core, lax.rem(self.own_second + k, side))
                )
            for k in range(side):
                self.arrived(self.second, self.second_sem, (1 - core, k))
            halves = []
            for half in range(2):
                values = [self.second[half, k] for k in range(side)]
                while len(values) > 1:
                    values = [p + q for p, q in zip(values[::2], values[1::2])]
                halves.append(values[0])
            return jnp.concatenate(halves, axis=0)

        def drain(self):
            for k in range(1, side):
                for half in range(2):
                    self.first_send(half, k).wait_send()
                    self.second_send(half, k).wait_send()
            self.first_partner().wait_send()
            self.second_partner().wait_send()

    channels, taken = [], 0
    for tiles in CHANNELS:
        channels.append([])
        for _ in tiles:
            channels[-1].append(Channel(channel_refs[taken : taken + 6]))
            taken += 6

    def drain(app):
        @pl.when(me < count - 1)
        def _():
            forward(app).wait_send()

        @pl.when(me > 0)
        def _():
            backward(app).wait_send()

        for channel in channels[app]:
            channel.drain()

    def wide(refs, group):
        return jnp.concatenate(
            [
                jnp.concatenate([ref[group * REACH + k + shift] for ref, shift in refs], axis=0)
                for k in range(REACH)
            ],
            axis=1,
        )

    def wide_row(ref, group):
        return jnp.concatenate(
            [ref[group * REACH + k : group * REACH + k + 1, :] for k in range(REACH)], axis=1
        )

    def late_block(app):
        ext = exts[app]
        acc = mm3(wide([(ext, REACH)], 0), wide([(stiff_new, 0)], 0), True)
        for g in range(1, groups):
            acc = acc + mm3(wide([(ext, REACH)], g), wide([(stiff_new, 0)], g), True)
        return acc

    for b in range(blocks + REACH):
        product[b, SLOTS] = jnp.zeros((MODES, WIDTH), jnp.float32)
    for copy in loads:
        copy.wait()
    acc = jnp.zeros((MODES, MODES), jnp.float32)
    for g in range(groups):
        left = wide([(ext0, REACH)], g)
        acc = acc + mm3(left * wide_row(mass, g), left, True)
    channels[0][0].store(pack32(acc))
    table_load.wait()
    for b in range(blocks):
        for d in range(1, REACH + 1):
            slot = SLOTS
            for s in range(SLOTS):
                slot = jnp.where(offsets[b, s] == d, s, slot)
            slot_of[b, d - 1] = slot
    for b in range(blocks, blocks + REACH):
        for d in range(REACH):
            slot_of[b, d] = SLOTS

    def ready(g):
        for copy in matrix_loads[g]:
            copy.wait()
        for b in range(g * REACH, (g + 1) * REACH):
            whole = jnp.concatenate([diag[b]] + [coupling[b, s] for s in range(SLOTS)], axis=1)
            high[b], low[b] = split(whole)

    def enter():
        pl.semaphore_wait(barrier, len(greeted))
        channels[0][0].start()

    apply_stiffness(0, ready, (enter, lambda: None))
    channels[0][1].store(pack32(late_block(0)))
    channels[0][1].start()
    identity = eye(WIDTH)
    for b in range(blocks):
        inverse_diag[b : b + 1, :] = 1.0 / jnp.sum(diag[b] * identity, axis=0, keepdims=True)
    channels[0][0].middle()
    channels[0][1].middle()
    factor = first_factor(unpack32(channels[0][0].finish()))
    block = unpack32(channels[0][1].finish())
    projected = mm_nt(mm(factor, block, HIGHEST), factor, HIGHEST)
    projected = 0.5 * (projected + projected.T)
    coefficients = factor
    basis, stiff_basis = [(ext0, REACH)], [(stiff_new, 0)]
    previous = None

    for step in range(1, ITERS + 1):
        ext = exts[step]
        order = coefficients.shape[1]
        later = jnp.where(lanes((MODES, order)) < MODES, 0.0, coefficients)
        moving = previous is not None
        both = jnp.concatenate([coefficients, later], axis=0) if moving else coefficients
        n = MODES * (3 if moving else 2)
        stiff_acc = jnp.zeros((MODES, n - MODES), jnp.float32)
        mass_acc = jnp.zeros((MODES, n), jnp.float32)
        for g in range(groups):
            new = mm3(both, wide(basis, g))
            stiff = mm3(both, wide(stiff_basis, g))
            masses = wide_row(mass, g)
            residual = stiff[:MODES] - mm3(projected[:, :MODES], new[:MODES] * masses)
            residual = residual * wide_row(inverse_diag, g)
            for k in range(REACH):
                b = g * REACH + k
                cut = slice(k * WIDTH, (k + 1) * WIDTH)
                modes[b] = new[:MODES, cut]
                stiff_modes[b] = stiff[:MODES, cut]
                ext[b + REACH] = residual[:, cut]
                if moving:
                    direction[b] = new[MODES:, cut]
                    stiff_direction[b] = stiff[MODES:, cut]
            right = [new[:MODES], residual] + ([new[MODES:]] if moving else [])
            mass_acc = mass_acc + mm3(residual * masses, jnp.concatenate(right, axis=0), True)
            stiff_acc = stiff_acc + mm3(residual, stiff, True)
        mass_sum, stiff_sum, late_sum = channels[step]
        mass_sum.store(pack96(mass_acc) if moving else pack64(mass_acc))
        stiff_sum.store(pack64(stiff_acc) if moving else pack32(stiff_acc))

        def leave(mass_sum=mass_sum, stiff_sum=stiff_sum):
            mass_sum.start()
            stiff_sum.start()

        apply_stiffness(step, lambda g: None, (leave, lambda: None))
        basis = [(modes, 0), (ext, REACH)] + ([(direction, 0)] if moving else [])
        stiff_basis = [(stiff_modes, 0), (stiff_new, 0)] + ([(stiff_direction, 0)] if moving else [])
        late_sum.store(pack32(late_block(step)))
        late_sum.start()
        shape = (MODES, n)
        lane = lanes(shape)
        unit = jnp.where(lane == sublanes(shape), 1.0, 0.0)
        placed = mm(0.5 * projected[:, :MODES], unit, HIGHEST)
        third = []
        if moving:
            zero = jnp.zeros((MODES, order), jnp.float32)
            spread_rows = jnp.concatenate([coefficients, zero, later], axis=0)
            third = [
                [
                    mm_nt(mm(later, old, HIGHEST), spread_rows, HIGHEST)
                    * jnp.where(lane < 2 * MODES, 1.0, 0.5)
                ]
                for old in previous
            ]
        else:
            third = [[], []]
        drain(step - 1)
        mass_sum.middle()
        stiff_sum.middle()
        late_sum.middle()
        early_mass = mass_sum.finish()
        early_mass = unpack96(early_mass) if moving else unpack64(early_mass)
        half = jnp.where((lane >= MODES) & (lane < 2 * MODES), 0.5, 1.0)
        gram_mass = jnp.concatenate([0.5 * unit, early_mass * half] + third[1], axis=0)
        gram_mass = gram_mass + gram_mass.T
        factor = next_factor(gram_mass)
        middle = factor[:, MODES : 2 * MODES]
        early_stiff = stiff_sum.finish()
        early_stiff = unpack64(early_stiff) if moving else unpack32(early_stiff)
        empty = jnp.zeros((MODES, MODES), jnp.float32)
        pieces = [early_stiff[:, :MODES], empty] + ([early_stiff[:, MODES:]] if moving else [])
        rest = jnp.concatenate([placed, jnp.concatenate(pieces, axis=1)] + third[0], axis=0)
        rest = rest + rest.T
        known = mm_nt(mm(factor, rest, HIGHEST), factor, HIGHEST)
        block = unpack32(late_sum.finish())
        reduced = known + mm_nt(mm(middle, block, HIGHEST), middle, HIGHEST)
        reduced = 0.5 * (reduced + reduced.T)
        coefficients, projected = ritz_rows(reduced, factor)
        if step < ITERS:
            spot = jnp.where(lane == sublanes(shape) + MODES, 1.0, 0.0)
            inner = [jnp.zeros(shape, jnp.float32), mm(block, spot, HIGHEST)]
            inner += [jnp.zeros(shape, jnp.float32)] * (n // MODES - 2)
            previous = [rest + jnp.concatenate(inner, axis=0), gram_mass]

    weight = count * blocks * WIDTH / MODES
    for g in range(groups):
        new = mm3(coefficients, wide(basis, g))
        stiff = mm3(coefficients, wide(stiff_basis, g))
        density = weight * wide_row(mass, g) * jnp.sum(new * new, axis=0, keepdims=True)
        energy = weight * jnp.sum(new * stiff, axis=0, keepdims=True)
        for k in range(REACH):
            cut = slice(k * WIDTH, (k + 1) * WIDTH)
            mass_out[g * REACH + k : g * REACH + k + 1, :] = density[:, cut]
            energy_out[g * REACH + k : g * REACH + k + 1, :] = energy[:, cut]
    drain(ITERS)


def solution(mesh):
    count = mesh.shape["row"]

    def local(diag_blocks, coupling, offsets, mass, initial_modes):
        blocks = diag_blocks.shape[0]
        apps = ITERS + 1
        side = TORUS[1]
        cores = TORUS[2]
        f32 = jnp.float32
        dma = pltpu.SemaphoreType.DMA
        vector = pltpu.VMEM((blocks, MODES, WIDTH), f32)
        extended = pltpu.VMEM((blocks + REACH, MODES, WIDTH), f32)
        halo = pltpu.VMEM((apps, REACH, MODES, WIDTH), f32)
        channel_shapes = []
        for tiles in CHANNELS:
            for tile in tiles:
                rows = 4 * tile
                channel_shapes += [
                    pltpu.VMEM((2, rows, WIDTH), f32),
                    pltpu.VMEM((side * cores, rows, WIDTH), f32),
                    pltpu.VMEM((2, side, rows, WIDTH), f32),
                    dma((2, 2, side)),
                    dma((side * cores,)),
                    dma((2, side)),
                ]
        outs = pl.pallas_call(
            lambda *refs: solve_kernel((count, blocks), *refs),
            out_shape=[jax.ShapeDtypeStruct((blocks, WIDTH), f32)] * 2,
            in_specs=[
                pl.BlockSpec(memory_space=pl.ANY),
                pl.BlockSpec(memory_space=pl.ANY),
                pl.BlockSpec(memory_space=pl.ANY),
                pl.BlockSpec(memory_space=pl.ANY),
                pl.BlockSpec(memory_space=pl.ANY),
            ],
            out_specs=[pl.BlockSpec(memory_space=pltpu.VMEM)] * 2,
            scratch_shapes=[
                pltpu.VMEM((blocks, WIDTH, WIDTH), f32),
                pltpu.VMEM((blocks, SLOTS, WIDTH, WIDTH), f32),
                pltpu.VMEM((blocks, WIDTH, (SLOTS + 1) * WIDTH), jnp.bfloat16),
                pltpu.VMEM((blocks, WIDTH, (SLOTS + 1) * WIDTH), jnp.bfloat16),
                pltpu.VMEM((blocks, WIDTH), f32),
                pltpu.SMEM((blocks, SLOTS), jnp.int32),
                pltpu.SMEM((blocks + REACH, REACH), jnp.int32),
                pltpu.VMEM((blocks, WIDTH), f32),
                pltpu.VMEM((blocks + REACH, SLOTS + 1, MODES, WIDTH), f32),
                extended,
                extended,
                extended,
                extended,
                vector,
                vector,
                vector,
                vector,
                vector,
                halo,
                halo,
                halo,
                dma((blocks + 2,)),
                dma((2, blocks // REACH)),
                dma((apps, 2)),
                dma((apps, 2)),
                *channel_shapes,
            ],
            compiler_params=pltpu.CompilerParams(
                collective_id=0, has_side_effects=True, vmem_limit_bytes=60 << 20
            ),
            name="lobpcg",
        )(diag_blocks, coupling, offsets, mass.reshape(blocks, WIDTH), initial_modes)
        return outs[0].reshape(-1), outs[1].reshape(-1)

    spec = ("sub", "row")
    return jax.shard_map(
        local,
        mesh=mesh,
        in_specs=(
            P(spec, None, None),
            P(spec, None, None, None),
            P(spec, None),
            P(spec),
            P(None, spec),
        ),
        out_specs=(P(spec), P(spec)),
        check_vma=False,
    )
```

```python
import jax
import jax.numpy as jnp
from jax import lax
from jax.experimental import pallas as pl
from jax.experimental.pallas import tpu as pltpu
from jax.sharding import PartitionSpec as P

MODES = 32
REACH = 4
SLOTS = 3
ITERS = 3
PURIFY = 28
WIDTH = 128
TORUS = (8, 8, 2)
MESH = pl.DeviceIdType.MESH
CHANNELS = ((1, 1), (2, 1, 1), (3, 2, 1), (3, 2, 1))

HIGHEST = lax.Precision.HIGHEST


def mm(a, b, precision):
    return lax.dot_general(
        a, b, (((1,), (0,)), ((), ())), precision=precision, preferred_element_type=jnp.float32
    )


def mm_nt(a, b, precision):
    return lax.dot_general(
        a, b, (((1,), (1,)), ((), ())), precision=precision, preferred_element_type=jnp.float32
    )


def split(value):
    high = value.astype(jnp.bfloat16)
    return high, (value - high.astype(jnp.float32)).astype(jnp.bfloat16)


def mm3(a, b, transposed=False):
    contract = (((1,), (1 if transposed else 0,)), ((), ()))
    a_high, a_low = split(a)
    b_high, b_low = b if isinstance(b, tuple) else split(b)
    rows = a.shape[0]
    top = lax.dot_general(
        jnp.concatenate([a_high, a_low], axis=0),
        b_high,
        contract,
        preferred_element_type=jnp.float32,
    )
    rest = lax.dot_general(a_high, b_low, contract, preferred_element_type=jnp.float32)
    return (top[:rows] + rest) + top[rows:]


def lanes(shape):
    return lax.broadcasted_iota(jnp.int32, shape, 1)


def sublanes(shape):
    return lax.broadcasted_iota(jnp.int32, shape, 0)


def eye(n):
    return (sublanes((n, n)) == lanes((n, n))).astype(jnp.float32)


def total(x):
    return jnp.sum(jnp.sum(x, axis=0, keepdims=True), axis=1, keepdims=True)


def inverse_factor(table, first):
    rows, cols = table.shape
    done = []
    for start in range(0, rows, 8):
        live = table.shape[0]
        column = [
            jnp.broadcast_to(table[:, first + start + k : first + start + k + 1], (live, cols))
            for k in range(8)
        ]
        index = sublanes((live, cols))
        lane = lanes((live, cols))
        for k in range(8):
            at = first + start + k
            pivot = column[k][k : k + 1, :]
            scale = lax.rsqrt(pivot)
            row = jnp.where(lane[0:1] == at, 1.0, table[k : k + 1, :]) * scale
            factor = jnp.where(index > k, column[k] * scale, 0.0)
            table = jnp.where((index > k) & (lane == at), 0.0, table) - factor * row
            table = jnp.where(index == k, row, table)
            for m in range(k + 1, 8):
                column[m] = column[m] - factor * (column[m][k : k + 1, :] * scale)
        done.append(table[:8])
        table = table[8:]
    result = jnp.concatenate(done, axis=0) if len(done) > 1 else done[0]
    shape = (rows, cols)
    return jnp.where(lanes(shape) <= sublanes(shape) + first, result, 0.0)


def purify(matrix):
    n = matrix.shape[0]
    identity = eye(n)
    diagonal = jnp.sum(matrix * identity, axis=0, keepdims=True)
    radius = jnp.sum(jnp.abs(matrix), axis=0, keepdims=True) - jnp.abs(diagonal)
    center = jnp.sum(diagonal, axis=1, keepdims=True) / n
    highest = jnp.max(diagonal + radius, axis=1, keepdims=True)
    lowest = jnp.min(diagonal - radius, axis=1, keepdims=True)
    factor = jnp.minimum(
        MODES / jnp.maximum(highest - center, 1e-6), (n - MODES) / jnp.maximum(center - lowest, 1e-6)
    )
    initial = factor / n * (center * identity - matrix) + MODES / n * identity

    def step(index, density):
        square = mm3(density, density)
        cube = mm3(square, density)
        denominator = total((density - square) * identity)
        numerator = total(square * (identity - density))
        safe = jnp.where(jnp.abs(denominator) > 1e-12, denominator, 1.0)
        ratio = jnp.clip(numerator / safe, 0.0, 1.0)
        up = ratio >= 0.5
        scale = 1.0 / jnp.maximum(jnp.where(up, ratio, 1.0 - ratio), 0.5)
        first = jnp.where(up, 0.0, (1.0 - 2.0 * ratio) * scale)
        second = (1.0 + ratio) * scale
        return first * density + second * square - scale * cube

    return lax.fori_loop(0, PURIFY, step, initial)


def pack32(block):
    return jnp.concatenate([block[8 * k : 8 * k + 8] for k in range(4)], axis=1)


def unpack32(tile):
    return jnp.concatenate([tile[:, MODES * k : MODES * (k + 1)] for k in range(4)], axis=0)


def pack64(block):
    return jnp.concatenate([block[:16], block[16:]], axis=1)


def unpack64(tile):
    return jnp.concatenate([tile[:, : 2 * MODES], tile[:, 2 * MODES :]], axis=0)


def pack96(block):
    last = [block[24:, MODES * k : MODES * (k + 1)] for k in range(3)]
    return jnp.concatenate([block[:24], jnp.concatenate(last, axis=0)], axis=1)


def unpack96(tile):
    last = [tile[8 * k : 8 * k + 8, 3 * MODES :] for k in range(3)]
    return jnp.concatenate([tile[:, : 3 * MODES], jnp.concatenate(last, axis=1)], axis=0)


def first_factor(gram_mass):
    return inverse_factor(0.5 * (gram_mass + gram_mass.T), 0)


def next_factor(gram_mass):
    n = gram_mass.shape[0]
    rest = n - MODES
    side = gram_mass[:, :MODES]
    side = jnp.where(sublanes((n, MODES)) < MODES, 0.0, side)
    lower = gram_mass[MODES:, :]
    schur = lower - mm_nt(side[MODES:], side, HIGHEST)
    bottom = inverse_factor(jnp.where(lanes((rest, n)) < MODES, -lower, schur), MODES)
    shape = (MODES, n)
    unit = jnp.where(lanes(shape) == sublanes(shape), 1.0, 0.0)
    return jnp.concatenate([unit, bottom], axis=0)


def ritz_rows(reduced, factor):
    rows = purify(reduced)[:MODES]
    change = inverse_factor(mm_nt(rows, rows, HIGHEST), 0)
    coefficients = mm(rows, factor, HIGHEST)
    projected = mm_nt(mm(rows, reduced, HIGHEST), rows, HIGHEST)
    coefficients = mm(change, coefficients, HIGHEST)
    projected = mm_nt(mm(change, projected, HIGHEST), change, HIGHEST)
    return coefficients, projected


def solve_kernel(
    sizes,
    diag_hbm,
    coupling_hbm,
    offsets_hbm,
    mass_hbm,
    initial_hbm,
    mass_out,
    energy_out,
    diag,
    coupling,
    high,
    low,
    mass,
    offsets,
    slot_of,
    inverse_diag,
    product,
    ext0,
    ext1,
    ext2,
    ext3,
    stiff_new,
    modes,
    stiff_modes,
    direction,
    stiff_direction,
    edge,
    landing,
    returned,
    load_sem,
    matrix_sem,
    halo_send,
    halo_recv,
    *channel_refs,
):
    count, blocks = sizes
    ny, nx, cores = TORUS
    side = nx
    me = lax.axis_index("row")
    core = lax.rem(me, cores)
    x = lax.rem(lax.div(me, cores), nx)
    y = lax.div(me, cores * nx)
    partner = me + 1 - 2 * core
    exts = (ext0, ext1, ext2, ext3)
    groups = blocks // REACH

    table_load = pltpu.make_async_copy(offsets_hbm, offsets, load_sem.at[blocks + 1])
    loads = [pltpu.make_async_copy(mass_hbm, mass, load_sem.at[blocks])]
    loads += [
        pltpu.make_async_copy(
            initial_hbm.at[:, pl.ds(b * WIDTH, WIDTH)], ext0.at[b + REACH], load_sem.at[b]
        )
        for b in range(blocks)
    ]
    matrix_loads = [
        [
            pltpu.make_async_copy(
                ref.at[pl.ds(g * REACH, REACH)], out.at[pl.ds(g * REACH, REACH)], matrix_sem.at[i, g]
            )
            for i, (ref, out) in enumerate([(diag_hbm, diag), (coupling_hbm, coupling)])
        ]
        for g in range(groups)
    ]
    table_load.start()
    for copy in loads:
        copy.start()
    for pair in matrix_loads:
        for copy in pair:
            copy.start()

    x_at = [lax.rem(x + k, nx) for k in range(side)]
    y_at = [lax.rem(y + k, ny) for k in range(side)]

    def device(px, py, pcore):
        return {"row": (py * nx + px) * cores + pcore}

    barrier = pltpu.get_barrier_semaphore()
    greeted = [{"row": partner}, {"row": lax.rem(me + 1, count)}, {"row": lax.rem(me + count - 1, count)}]
    for k in range(1, side):
        for pcore in range(cores):
            greeted += [device(x_at[k], y, pcore), device(x, y_at[k], pcore)]
    for other in greeted:
        pl.semaphore_signal(barrier, inc=1, device_id=other, device_id_type=MESH)

    def send(source, target, send_sem, recv_sem, other):
        return pltpu.make_async_remote_copy(
            src_ref=source,
            dst_ref=target,
            send_sem=send_sem,
            recv_sem=recv_sem,
            device_id=other,
            device_id_type=MESH,
        )

    def forward(app):
        return send(
            exts[app].at[pl.ds(blocks, REACH)],
            landing.at[app],
            halo_send.at[app, 0],
            halo_recv.at[app, 0],
            {"row": me + 1},
        )

    def backward(app):
        return send(
            edge.at[app],
            returned.at[app],
            halo_send.at[app, 1],
            halo_recv.at[app, 1],
            {"row": me - 1},
        )

    def own_products(ext, b):
        out = mm3(ext[b + REACH], (high[b], low[b]))
        stiff_new[b] = out[:, :WIDTH]
        for s in range(SLOTS):
            product[b, s] = out[:, (s + 1) * WIDTH : (s + 2) * WIDTH]

    def other_products(ext, b):
        taken = jnp.concatenate([ext[b + REACH - offsets[s, b]] for s in range(SLOTS)], axis=1)
        spread = [product[b + d, slot_of[b + d, d - 1]] for d in range(1, REACH + 1)]
        spread = (spread[0] + spread[1]) + (spread[2] + spread[3])
        out = mm3(taken, (high[b, :, WIDTH:], low[b, :, WIDTH:]), True)
        stiff_new[b] = stiff_new[b] + out + spread

    def send_forward(app):
        @pl.when(me < count - 1)
        def _():
            forward(app).start()

    def send_backward(app):
        for e in range(REACH):
            out = jnp.zeros((MODES, WIDTH), jnp.float32)
            for b in range(e + 1):
                out = out + product[b, slot_of[b, b - e + REACH - 1]]
            edge[app, e] = out

        @pl.when(me > 0)
        def _():
            backward(app).start()

    def late_part(app, g):
        return mm3(wide([(exts[app], REACH)], g), wide([(stiff_new, 0)], g), True)

    def rest_of_product(app, ready):
        ext = exts[app]
        for g in range(1, groups):
            ready(g)
            for b in range(g * REACH, (g + 1) * REACH):
                own_products(ext, b)
        for b in range(REACH, blocks):
            other_products(ext, b)
        acc = late_part(app, 1)
        for g in range(2, groups - 1):
            acc = acc + late_part(app, g)

        @pl.when(me > 0)
        def _():
            forward(app).wait_recv()
            ext[0:REACH] = landing[app]

        @pl.when(me == 0)
        def _():
            ext[0:REACH] = jnp.zeros((REACH, MODES, WIDTH), jnp.float32)

        for b in range(REACH):
            other_products(ext, b)
        acc = acc + late_part(app, 0)

        @pl.when(me < count - 1)
        def _():
            backward(app).wait_recv()
            for k in range(REACH):
                b = blocks - REACH + k
                stiff_new[b] = stiff_new[b] + returned[app, k]

        return acc + late_part(app, groups - 1)

    class Channel:
        def __init__(self, refs):
            (self.part, self.first, self.second, self.sends, self.first_sem, self.second_sem) = refs
            self.own_first = (x * (1 - core) + y * core) * cores + core
            self.own_second = y * (1 - core) + x * core

        def first_send(self, half, k):
            if half == 0:
                slot, target = x * cores + core, device(x_at[k], y, 0)
            else:
                slot, target = y * cores + core, device(x, y_at[k], 1)
            return send(
                self.part.at[half],
                self.first.at[slot],
                self.sends.at[0, half, k],
                self.first_sem.at[slot],
                target,
            )

        def first_partner(self):
            half = 1 - core
            slot = (x * core + y * half) * cores + core
            return send(
                self.part.at[half],
                self.first.at[slot],
                self.sends.at[0, half, 0],
                self.first_sem.at[slot],
                {"row": partner},
            )

        def second_send(self, pcore, k):
            where = self.own_second
            px = x * (1 - core) + x_at[k] * core
            py = y_at[k] * (1 - core) + y * core
            return send(
                self.second.at[core, where],
                self.second.at[core, where],
                self.sends.at[1, pcore, k],
                self.second_sem.at[core, where],
                device(px, py, pcore),
            )

        def second_partner(self):
            where = self.own_second
            return send(
                self.second.at[core, where],
                self.second.at[core, where],
                self.sends.at[1, 1 - core, 0],
                self.second_sem.at[core, where],
                {"row": partner},
            )

        def arrived(self, buffer, sem, index):
            send(
                buffer.at[index], buffer.at[index], self.sends.at[0, 0, 0], sem.at[index],
                {"row": partner},
            ).wait_recv()

        def store(self, packed):
            rows = packed.shape[0] // 2
            self.part[0] = packed[:rows]
            self.part[1] = packed[rows:]

        def start(self):
            self.first[self.own_first] = self.part[core]
            for k in range(1, side):
                for half in range(2):
                    self.first_send(half, k).start()
            self.first_partner().start()

        def middle(self):
            slots = side * cores
            for k in range(1, slots):
                self.arrived(self.first, self.first_sem, lax.rem(self.own_first + k, slots))
            values = [self.first[k] for k in range(slots)]
            while len(values) > 1:
                values = [p + q for p, q in zip(values[::2], values[1::2])]
            self.second[core, self.own_second] = values[0]
            for k in range(1, side):
                for pcore in range(cores):
                    self.second_send(pcore, k).start()
            self.second_partner().start()

        def finish(self):
            for k in range(1, side):
                self.arrived(
                    self.second, self.second_sem, (core, lax.rem(self.own_second + k, side))
                )
            for k in range(side):
                self.arrived(self.second, self.second_sem, (1 - core, k))
            halves = []
            for half in range(2):
                values = [self.second[half, k] for k in range(side)]
                while len(values) > 1:
                    values = [p + q for p, q in zip(values[::2], values[1::2])]
                halves.append(values[0])
            return jnp.concatenate(halves, axis=0)

        def drain(self):
            for k in range(1, side):
                for half in range(2):
                    self.first_send(half, k).wait_send()
                    self.second_send(half, k).wait_send()
            self.first_partner().wait_send()
            self.second_partner().wait_send()

    channels, taken = [], 0
    for tiles in CHANNELS:
        channels.append([])
        for _ in tiles:
            channels[-1].append(Channel(channel_refs[taken : taken + 6]))
            taken += 6

    def drain(app):
        @pl.when(me < count - 1)
        def _():
            forward(app).wait_send()

        @pl.when(me > 0)
        def _():
            backward(app).wait_send()

        for channel in channels[app]:
            channel.drain()

    def wide(refs, group):
        return jnp.concatenate(
            [
                jnp.concatenate([ref[group * REACH + k + shift] for ref, shift in refs], axis=0)
                for k in range(REACH)
            ],
            axis=1,
        )

    def wide_row(ref, group):
        return jnp.concatenate(
            [ref[group * REACH + k : group * REACH + k + 1, :] for k in range(REACH)], axis=1
        )

    for b in range(blocks + REACH):
        product[b, SLOTS] = jnp.zeros((MODES, WIDTH), jnp.float32)
    for copy in loads:
        copy.wait()
    acc = jnp.zeros((MODES, MODES), jnp.float32)
    for g in range(groups):
        left = wide([(ext0, REACH)], g)
        acc = acc + mm3(left * wide_row(mass, g), left, True)
    channels[0][0].store(pack32(acc))
    table_load.wait()
    for b in range(blocks):
        for d in range(1, REACH + 1):
            slot = SLOTS
            for s in range(SLOTS):
                slot = jnp.where(offsets[s, b] == d, s, slot)
            slot_of[b, d - 1] = slot
    for b in range(blocks, blocks + REACH):
        for d in range(REACH):
            slot_of[b, d] = SLOTS

    def ready(g):
        for copy in matrix_loads[g]:
            copy.wait()
        for b in range(g * REACH, (g + 1) * REACH):
            whole = jnp.concatenate([diag[b]] + [coupling[b, s] for s in range(SLOTS)], axis=1)
            high[b], low[b] = split(whole)

    ready(0)
    for b in range(REACH):
        own_products(ext0, b)
    pl.semaphore_wait(barrier, len(greeted))
    send_forward(0)
    send_backward(0)
    channels[0][0].start()
    channels[0][1].store(pack32(rest_of_product(0, ready)))
    channels[0][1].start()
    identity = eye(WIDTH)
    for b in range(blocks):
        inverse_diag[b : b + 1, :] = 1.0 / jnp.sum(diag[b] * identity, axis=0, keepdims=True)
    channels[0][0].middle()
    channels[0][1].middle()
    factor = first_factor(unpack32(channels[0][0].finish()))
    block = unpack32(channels[0][1].finish())
    projected = mm_nt(mm(factor, block, HIGHEST), factor, HIGHEST)
    projected = 0.5 * (projected + projected.T)
    coefficients = factor
    basis, stiff_basis = [(ext0, REACH)], [(stiff_new, 0)]
    previous = None

    for step in range(1, ITERS + 1):
        ext = exts[step]
        order = coefficients.shape[1]
        later = jnp.where(lanes((MODES, order)) < MODES, 0.0, coefficients)
        moving = previous is not None
        both = jnp.concatenate([coefficients, later], axis=0) if moving else coefficients
        n = MODES * (3 if moving else 2)
        stiff_acc = jnp.zeros((MODES, n - MODES), jnp.float32)
        mass_acc = jnp.zeros((MODES, n), jnp.float32)
        for g in (groups - 1, 0, *range(1, groups - 1)):
            new = mm3(both, wide(basis, g))
            stiff = mm3(both, wide(stiff_basis, g))
            masses = wide_row(mass, g)
            residual = stiff[:MODES] - mm3(projected, new[:MODES] * masses)
            residual = residual * wide_row(inverse_diag, g)
            for k in range(REACH):
                b = g * REACH + k
                cut = slice(k * WIDTH, (k + 1) * WIDTH)
                modes[b] = new[:MODES, cut]
                stiff_modes[b] = stiff[:MODES, cut]
                ext[b + REACH] = residual[:, cut]
                if moving:
                    direction[b] = new[MODES:, cut]
                    stiff_direction[b] = stiff[MODES:, cut]
            right = [new[:MODES], residual] + ([new[MODES:]] if moving else [])
            mass_acc = mass_acc + mm3(residual * masses, jnp.concatenate(right, axis=0), True)
            stiff_acc = stiff_acc + mm3(residual, stiff, True)
            if g == 0:
                for b in range(REACH):
                    own_products(ext, b)
                send_forward(step)
                send_backward(step)
        mass_sum, stiff_sum, late_sum = channels[step]
        mass_sum.store(pack96(mass_acc) if moving else pack64(mass_acc))
        stiff_sum.store(pack64(stiff_acc) if moving else pack32(stiff_acc))
        mass_sum.start()
        stiff_sum.start()
        late_sum.store(pack32(rest_of_product(step, lambda g: None)))
        late_sum.start()
        basis = [(modes, 0), (ext, REACH)] + ([(direction, 0)] if moving else [])
        stiff_basis = [(stiff_modes, 0), (stiff_new, 0)] + ([(stiff_direction, 0)] if moving else [])
        shape = (MODES, n)
        lane = lanes(shape)
        unit = jnp.where(lane == sublanes(shape), 1.0, 0.0)
        placed = mm(0.5 * projected, unit, HIGHEST)
        third = []
        if moving:
            zero = jnp.zeros((MODES, order), jnp.float32)
            spread_rows = jnp.concatenate([coefficients, zero, later], axis=0)
            third = [
                [
                    mm_nt(mm(later, old, HIGHEST), spread_rows, HIGHEST)
                    * jnp.where(lane < 2 * MODES, 1.0, 0.5)
                ]
                for old in previous
            ]
        else:
            third = [[], []]
        drain(step - 1)
        mass_sum.middle()
        stiff_sum.middle()
        late_sum.middle()
        early_mass = mass_sum.finish()
        early_mass = unpack96(early_mass) if moving else unpack64(early_mass)
        half = jnp.where((lane >= MODES) & (lane < 2 * MODES), 0.5, 1.0)
        gram_mass = jnp.concatenate([0.5 * unit, early_mass * half] + third[1], axis=0)
        gram_mass = gram_mass + gram_mass.T
        factor = next_factor(gram_mass)
        middle = factor[:, MODES : 2 * MODES]
        early_stiff = stiff_sum.finish()
        early_stiff = unpack64(early_stiff) if moving else unpack32(early_stiff)
        empty = jnp.zeros((MODES, MODES), jnp.float32)
        pieces = [early_stiff[:, :MODES], empty] + ([early_stiff[:, MODES:]] if moving else [])
        rest = jnp.concatenate([placed, jnp.concatenate(pieces, axis=1)] + third[0], axis=0)
        rest = rest + rest.T
        known = mm_nt(mm(factor, rest, HIGHEST), factor, HIGHEST)
        block = unpack32(late_sum.finish())
        reduced = known + mm_nt(mm(middle, block, HIGHEST), middle, HIGHEST)
        coefficients, projected = ritz_rows(reduced, factor)
        if step < ITERS:
            spot = jnp.where(lane == sublanes(shape) + MODES, 1.0, 0.0)
            inner = [jnp.zeros(shape, jnp.float32), mm(block, spot, HIGHEST)]
            inner += [jnp.zeros(shape, jnp.float32)] * (n // MODES - 2)
            previous = [rest + jnp.concatenate(inner, axis=0), gram_mass]

    weight = count * blocks * WIDTH / MODES
    for g in range(groups):
        new = mm3(coefficients, wide(basis, g))
        stiff = mm3(coefficients, wide(stiff_basis, g))
        density = weight * wide_row(mass, g) * jnp.sum(new * new, axis=0, keepdims=True)
        energy = weight * jnp.sum(new * stiff, axis=0, keepdims=True)
        for k in range(REACH):
            cut = slice(k * WIDTH, (k + 1) * WIDTH)
            mass_out[g * REACH + k : g * REACH + k + 1, :] = density[:, cut]
            energy_out[g * REACH + k : g * REACH + k + 1, :] = energy[:, cut]
    drain(ITERS)


def solution(mesh):
    count = mesh.shape["row"]

    def local(diag_blocks, coupling, offsets, mass, initial_modes):
        blocks = diag_blocks.shape[0]
        apps = ITERS + 1
        side = TORUS[1]
        cores = TORUS[2]
        f32 = jnp.float32
        dma = pltpu.SemaphoreType.DMA
        vector = pltpu.VMEM((blocks, MODES, WIDTH), f32)
        extended = pltpu.VMEM((blocks + REACH, MODES, WIDTH), f32)
        halo = pltpu.VMEM((apps, REACH, MODES, WIDTH), f32)
        channel_shapes = []
        for tiles in CHANNELS:
            for tile in tiles:
                rows = 4 * tile
                channel_shapes += [
                    pltpu.VMEM((2, rows, WIDTH), f32),
                    pltpu.VMEM((side * cores, rows, WIDTH), f32),
                    pltpu.VMEM((2, side, rows, WIDTH), f32),
                    dma((2, 2, side)),
                    dma((side * cores,)),
                    dma((2, side)),
                ]
        outs = pl.pallas_call(
            lambda *refs: solve_kernel((count, blocks), *refs),
            out_shape=[jax.ShapeDtypeStruct((blocks, WIDTH), f32)] * 2,
            in_specs=[
                pl.BlockSpec(memory_space=pltpu.HBM),
                pl.BlockSpec(memory_space=pltpu.HBM),
                pl.BlockSpec(memory_space=pltpu.HBM),
                pl.BlockSpec(memory_space=pltpu.HBM),
                pl.BlockSpec(memory_space=pltpu.HBM),
            ],
            out_specs=[pl.BlockSpec(memory_space=pltpu.VMEM)] * 2,
            scratch_shapes=[
                pltpu.VMEM((blocks, WIDTH, WIDTH), f32),
                pltpu.VMEM((blocks, SLOTS, WIDTH, WIDTH), f32),
                pltpu.VMEM((blocks, WIDTH, (SLOTS + 1) * WIDTH), jnp.bfloat16),
                pltpu.VMEM((blocks, WIDTH, (SLOTS + 1) * WIDTH), jnp.bfloat16),
                pltpu.VMEM((blocks, WIDTH), f32),
                pltpu.SMEM((SLOTS, blocks), jnp.int32),
                pltpu.SMEM((blocks + REACH, REACH), jnp.int32),
                pltpu.VMEM((blocks, WIDTH), f32),
                pltpu.VMEM((blocks + REACH, SLOTS + 1, MODES, WIDTH), f32),
                extended,
                extended,
                extended,
                extended,
                vector,
                vector,
                vector,
                vector,
                vector,
                halo,
                halo,
                halo,
                dma((blocks + 2,)),
                dma((2, blocks // REACH)),
                dma((apps, 2)),
                dma((apps, 2)),
                *channel_shapes,
            ],
            compiler_params=pltpu.CompilerParams(
                collective_id=0, has_side_effects=True, vmem_limit_bytes=56 << 20
            ),
            name="lobpcg",
        )(diag_blocks, coupling, offsets.T, mass.reshape(blocks, WIDTH), initial_modes)
        return outs[0].reshape(-1), outs[1].reshape(-1)

    spec = ("sub", "row")
    return jax.shard_map(
        local,
        mesh=mesh,
        in_specs=(
            P(spec, None, None),
            P(spec, None, None, None),
            P(spec, None),
            P(spec),
            P(None, spec),
        ),
        out_specs=(P(spec), P(spec)),
        check_vma=False,
    )
```

```python
import jax
import jax.numpy as jnp
from jax import lax
from jax.experimental import pallas as pl
from jax.experimental.pallas import tpu as pltpu
from jax.sharding import PartitionSpec as P

MODES = 32
REACH = 4
SLOTS = 3
ITERS = 3
PURIFY = 28
WIDTH = 128
TORUS = (8, 8, 2)
MESH = pl.DeviceIdType.MESH
CHANNELS = ((1, 1), (2, 1, 1), (3, 2, 1), (3, 2, 1))

HIGHEST = lax.Precision.HIGHEST


def mm(a, b, precision):
    return lax.dot_general(
        a, b, (((1,), (0,)), ((), ())), precision=precision, preferred_element_type=jnp.float32
    )


def mm_nt(a, b, precision):
    return lax.dot_general(
        a, b, (((1,), (1,)), ((), ())), precision=precision, preferred_element_type=jnp.float32
    )


def split(value):
    high = value.astype(jnp.bfloat16)
    return high, (value - high.astype(jnp.float32)).astype(jnp.bfloat16)


def mm3(a, b, transposed=False):
    contract = (((1,), (1 if transposed else 0,)), ((), ()))
    a_high, a_low = split(a)
    b_high, b_low = b if isinstance(b, tuple) else split(b)
    rows = a.shape[0]
    top = lax.dot_general(
        jnp.concatenate([a_high, a_low], axis=0),
        b_high,
        contract,
        preferred_element_type=jnp.float32,
    )
    rest = lax.dot_general(a_high, b_low, contract, preferred_element_type=jnp.float32)
    return (top[:rows] + rest) + top[rows:]


def lanes(shape):
    return lax.broadcasted_iota(jnp.int32, shape, 1)


def sublanes(shape):
    return lax.broadcasted_iota(jnp.int32, shape, 0)


def eye(n):
    return (sublanes((n, n)) == lanes((n, n))).astype(jnp.float32)


def total(x):
    return jnp.sum(jnp.sum(x, axis=0, keepdims=True), axis=1, keepdims=True)


def inverse_factor(table, first, halfway=lambda: None):
    rows, cols = table.shape
    index = sublanes((8, cols))
    lane = lanes((1, cols))
    done = []
    below = table
    for start in range(0, rows, 8):
        if start == rows // 2:
            halfway()
        at = first + start
        top, below = below[:8], below[8:]
        parts = [top] + ([below] if below.shape[0] else [])
        columns = [
            [jnp.broadcast_to(part[:, at + k : at + k + 1], part.shape) for part in parts]
            for k in range(8)
        ]
        panel = (lane >= at) & (lane < at + 8)
        parts = [jnp.where(panel, 0.0, part) for part in parts]
        for k in range(0, 8, 2):
            one, two = columns[k], columns[k + 1]
            a, c = one[0][k : k + 1, :], two[0][k + 1 : k + 2, :]
            b = one[0][k + 1 : k + 2, :]
            scale = lax.rsqrt(a)
            rest = lax.rsqrt(a * c - b * b)
            scale_two = a * scale * rest
            cross = b * scale * rest
            row = (parts[0][k : k + 1, :] + jnp.where(lane == at + k, 1.0, 0.0)) * scale
            row_two = (
                parts[0][k + 1 : k + 2, :] + jnp.where(lane == at + k + 1, 1.0, 0.0)
            ) * scale_two - cross * (parts[0][k : k + 1, :] + jnp.where(lane == at + k, 1.0, 0.0))
            factors = [column * scale for column in one]
            factors_two = [q * scale_two - p * cross for p, q in zip(one, two)]
            factors[0] = jnp.where(index > k + 1, factors[0], 0.0)
            factors_two[0] = jnp.where(index > k + 1, factors_two[0], 0.0)
            parts = [
                part - f * row - g * row_two for part, f, g in zip(parts, factors, factors_two)
            ]
            parts[0] = jnp.where(index == k, row, jnp.where(index == k + 1, row_two, parts[0]))
            for m in range(k + 2, 8):
                entry = columns[m][0][k : k + 1, :] * scale
                entry_two = columns[m][0][k + 1 : k + 2, :] * scale_two - cross * columns[m][0][k : k + 1, :]
                columns[m] = [
                    c_ - f * entry - g * entry_two
                    for c_, f, g in zip(columns[m], factors, factors_two)
                ]
        done.append(parts[0])
        below = parts[-1]
    result = jnp.concatenate(done, axis=0)
    shape = (rows, cols)
    return jnp.where(lanes(shape) <= sublanes(shape) + first, result, 0.0)


def purify(matrix):
    n = matrix.shape[0]
    identity = eye(n)
    diagonal = jnp.sum(matrix * identity, axis=0, keepdims=True)
    radius = jnp.sum(jnp.abs(matrix), axis=0, keepdims=True) - jnp.abs(diagonal)
    center = jnp.sum(diagonal, axis=1, keepdims=True) / n
    highest = jnp.max(diagonal + radius, axis=1, keepdims=True)
    lowest = jnp.min(diagonal - radius, axis=1, keepdims=True)
    factor = jnp.minimum(
        MODES / jnp.maximum(highest - center, 1e-6), (n - MODES) / jnp.maximum(center - lowest, 1e-6)
    )
    initial = factor / n * (center * identity - matrix) + MODES / n * identity
    edge = jnp.zeros((n, WIDTH - n), jnp.float32)
    initial = jnp.concatenate([initial, edge], axis=1)
    identity = jnp.where(lanes((n, WIDTH)) == sublanes((n, WIDTH)), 1.0, 0.0)
    fill = jnp.zeros((WIDTH - n, WIDTH), jnp.bfloat16)
    empty = jnp.zeros((WIDTH, WIDTH), jnp.bfloat16)

    def step(index, density):
        high, low = [jnp.concatenate([part, fill], axis=0) for part in split(density)]
        weights = jnp.concatenate(
            [jnp.concatenate([high, low], axis=1), jnp.concatenate([high, empty], axis=1)], axis=0
        )

        def times_density(value):
            both = lax.dot_general(
                jnp.concatenate(split(value), axis=1),
                weights,
                (((1,), (0,)), ((), ())),
                preferred_element_type=jnp.float32,
            )
            return both[:, :WIDTH] + both[:, WIDTH:]

        square = times_density(density)
        cube = times_density(square)
        denominator = total((density - square) * identity)
        numerator = total(square * (identity - density))
        safe = jnp.where(jnp.abs(denominator) > 1e-12, denominator, 1.0)
        ratio = jnp.clip(numerator / safe, 0.0, 1.0)
        up = ratio >= 0.5
        scale = 1.0 / jnp.maximum(jnp.where(up, ratio, 1.0 - ratio), 0.5)
        first = jnp.where(up, 0.0, (1.0 - 2.0 * ratio) * scale)
        second = (1.0 + ratio) * scale
        return first * density + second * square - scale * cube

    return lax.fori_loop(0, PURIFY, step, initial)[:MODES, :n]


def pack32(block):
    return jnp.concatenate([block[8 * k : 8 * k + 8] for k in range(4)], axis=1)


def unpack32(tile):
    return jnp.concatenate([tile[:, MODES * k : MODES * (k + 1)] for k in range(4)], axis=0)


def pack64(block):
    return jnp.concatenate([block[:16], block[16:]], axis=1)


def unpack64(tile):
    return jnp.concatenate([tile[:, : 2 * MODES], tile[:, 2 * MODES :]], axis=0)


def pack96(block):
    last = [block[24:, MODES * k : MODES * (k + 1)] for k in range(3)]
    return jnp.concatenate([block[:24], jnp.concatenate(last, axis=0)], axis=1)


def unpack96(tile):
    last = [tile[8 * k : 8 * k + 8, 3 * MODES :] for k in range(3)]
    return jnp.concatenate([tile[:, : 3 * MODES], jnp.concatenate(last, axis=1)], axis=0)


def first_factor(gram_mass):
    return inverse_factor(0.5 * (gram_mass + gram_mass.T), 0)


def next_factor(gram_mass, halfway):
    n = gram_mass.shape[0]
    rest = n - MODES
    side = gram_mass[:, :MODES]
    side = jnp.where(sublanes((n, MODES)) < MODES, 0.0, side)
    lower = gram_mass[MODES:, :]
    schur = lower - mm_nt(side[MODES:], side, HIGHEST)
    bottom = inverse_factor(jnp.where(lanes((rest, n)) < MODES, -lower, schur), MODES, halfway)
    shape = (MODES, n)
    unit = jnp.where(lanes(shape) == sublanes(shape), 1.0, 0.0)
    return jnp.concatenate([unit, bottom], axis=0)


def ritz_rows(reduced, factor):
    rows = purify(reduced)
    change = inverse_factor(mm_nt(rows, rows, HIGHEST), 0)
    coefficients = mm(rows, factor, HIGHEST)
    projected = mm_nt(mm(rows, reduced, HIGHEST), rows, HIGHEST)
    coefficients = mm(change, coefficients, HIGHEST)
    projected = mm_nt(mm(change, projected, HIGHEST), change, HIGHEST)
    return coefficients, projected


def solve_kernel(
    sizes,
    diag_hbm,
    coupling_hbm,
    offsets_hbm,
    mass_hbm,
    initial_hbm,
    out,
    diag,
    coupling,
    high,
    low,
    mass,
    offsets,
    slot_of,
    inverse_diag,
    product,
    ext0,
    ext1,
    ext2,
    ext3,
    stiff_new,
    modes,
    stiff_modes,
    direction,
    stiff_direction,
    edge,
    landing,
    returned,
    load_sem,
    matrix_sem,
    halo_send,
    halo_recv,
    *channel_refs,
):
    count, blocks = sizes
    ny, nx, cores = TORUS
    side = nx
    me = lax.axis_index("row")
    core = lax.rem(me, cores)
    x = lax.rem(lax.div(me, cores), nx)
    y = lax.div(me, cores * nx)
    partner = me + 1 - 2 * core
    exts = (ext0, ext1, ext2, ext3)
    groups = blocks // REACH

    table_load = pltpu.make_async_copy(offsets_hbm, offsets, load_sem.at[blocks + 1])
    loads = [pltpu.make_async_copy(mass_hbm, mass, load_sem.at[blocks])]
    loads += [
        pltpu.make_async_copy(
            initial_hbm.at[:, pl.ds(b * WIDTH, WIDTH)], ext0.at[b + REACH], load_sem.at[b]
        )
        for b in range(blocks)
    ]
    matrix_loads = [
        [
            pltpu.make_async_copy(
                ref.at[pl.ds(g * REACH, REACH)], out.at[pl.ds(g * REACH, REACH)], matrix_sem.at[i, g]
            )
            for i, (ref, out) in enumerate([(diag_hbm, diag), (coupling_hbm, coupling)])
        ]
        for g in range(groups)
    ]
    table_load.start()
    for copy in loads:
        copy.start()
    for pair in matrix_loads:
        for copy in pair:
            copy.start()

    x_at = [lax.rem(x + k, nx) for k in range(side)]
    y_at = [lax.rem(y + k, ny) for k in range(side)]

    def device(px, py, pcore):
        return {"row": (py * nx + px) * cores + pcore}

    barrier = pltpu.get_barrier_semaphore()
    greeted = [{"row": partner}, {"row": lax.rem(me + 1, count)}, {"row": lax.rem(me + count - 1, count)}]
    for k in range(1, side):
        for pcore in range(cores):
            greeted += [device(x_at[k], y, pcore), device(x, y_at[k], pcore)]
    for other in greeted:
        pl.semaphore_signal(barrier, inc=1, device_id=other, device_id_type=MESH)

    def send(source, target, send_sem, recv_sem, other):
        return pltpu.make_async_remote_copy(
            src_ref=source,
            dst_ref=target,
            send_sem=send_sem,
            recv_sem=recv_sem,
            device_id=other,
            device_id_type=MESH,
        )

    def forward(app):
        return send(
            exts[app].at[pl.ds(blocks, REACH)],
            landing.at[app],
            halo_send.at[app, 0],
            halo_recv.at[app, 0],
            {"row": me + 1},
        )

    def backward(app):
        return send(
            edge.at[app],
            returned.at[app],
            halo_send.at[app, 1],
            halo_recv.at[app, 1],
            {"row": me - 1},
        )

    def own_products(ext, b):
        out = mm3(ext[b + REACH], (high[b], low[b]))
        stiff_new[b] = out[:, :WIDTH]
        for s in range(SLOTS):
            product[b, s] = out[:, (s + 1) * WIDTH : (s + 2) * WIDTH]

    def other_products(ext, b):
        taken = jnp.concatenate([ext[b + REACH - offsets[s, b]] for s in range(SLOTS)], axis=1)
        spread = [product[b + d, slot_of[b + d, d - 1]] for d in range(1, REACH + 1)]
        spread = (spread[0] + spread[1]) + (spread[2] + spread[3])
        out = mm3(taken, (high[b, :, WIDTH:], low[b, :, WIDTH:]), True)
        stiff_new[b] = stiff_new[b] + out + spread

    def send_forward(app):
        @pl.when(me < count - 1)
        def _():
            forward(app).start()

    def send_backward(app):
        for e in range(REACH):
            out = jnp.zeros((MODES, WIDTH), jnp.float32)
            for b in range(e + 1):
                out = out + product[b, slot_of[b, b - e + REACH - 1]]
            edge[app, e] = out

        @pl.when(me > 0)
        def _():
            backward(app).start()

    def late_part(app, g):
        return mm3(wide([(exts[app], REACH)], g), wide([(stiff_new, 0)], g), True)

    def rest_of_product(app, ready):
        ext = exts[app]
        for g in range(1, groups):
            ready(g)
            for b in range(g * REACH, (g + 1) * REACH):
                own_products(ext, b)
        for b in range(REACH, blocks):
            other_products(ext, b)
        acc = late_part(app, 1)
        for g in range(2, groups - 1):
            acc = acc + late_part(app, g)

        @pl.when(me > 0)
        def _():
            forward(app).wait_recv()
            ext[0:REACH] = landing[app]

        @pl.when(me == 0)
        def _():
            ext[0:REACH] = jnp.zeros((REACH, MODES, WIDTH), jnp.float32)

        for b in range(REACH):
            other_products(ext, b)
        acc = acc + late_part(app, 0)

        @pl.when(me < count - 1)
        def _():
            backward(app).wait_recv()
            for k in range(REACH):
                b = blocks - REACH + k
                stiff_new[b] = stiff_new[b] + returned[app, k]

        return acc + late_part(app, groups - 1)

    class Channel:
        def __init__(self, refs):
            (self.part, self.first, self.second, self.sends, self.first_sem, self.second_sem) = refs
            self.own_first = (x * (1 - core) + y * core) * cores + core
            self.own_second = y * (1 - core) + x * core

        def first_send(self, half, k):
            if half == 0:
                slot, target = x * cores + core, device(x_at[k], y, 0)
            else:
                slot, target = y * cores + core, device(x, y_at[k], 1)
            return send(
                self.part.at[half],
                self.first.at[slot],
                self.sends.at[0, half, k],
                self.first_sem.at[slot],
                target,
            )

        def first_partner(self):
            half = 1 - core
            slot = (x * core + y * half) * cores + core
            return send(
                self.part.at[half],
                self.first.at[slot],
                self.sends.at[0, half, 0],
                self.first_sem.at[slot],
                {"row": partner},
            )

        def second_send(self, pcore, k):
            where = self.own_second
            px = x * (1 - core) + x_at[k] * core
            py = y_at[k] * (1 - core) + y * core
            return send(
                self.second.at[core, where],
                self.second.at[core, where],
                self.sends.at[1, pcore, k],
                self.second_sem.at[core, where],
                device(px, py, pcore),
            )

        def second_partner(self):
            where = self.own_second
            return send(
                self.second.at[core, where],
                self.second.at[core, where],
                self.sends.at[1, 1 - core, 0],
                self.second_sem.at[core, where],
                {"row": partner},
            )

        def arrived(self, buffer, sem, index):
            send(
                buffer.at[index], buffer.at[index], self.sends.at[0, 0, 0], sem.at[index],
                {"row": partner},
            ).wait_recv()

        def store(self, packed):
            rows = packed.shape[0] // 2
            self.part[0] = packed[:rows]
            self.part[1] = packed[rows:]

        def start(self):
            self.first[self.own_first] = self.part[core]
            for k in range(1, side):
                for half in range(2):
                    self.first_send(half, k).start()
            self.first_partner().start()

        def middle(self):
            slots = side * cores
            for k in range(1, slots):
                self.arrived(self.first, self.first_sem, lax.rem(self.own_first + k, slots))
            values = [self.first[k] for k in range(slots)]
            while len(values) > 1:
                values = [p + q for p, q in zip(values[::2], values[1::2])]
            self.second[core, self.own_second] = values[0]
            for k in range(1, side):
                for pcore in range(cores):
                    self.second_send(pcore, k).start()
            self.second_partner().start()

        def finish(self):
            for k in range(1, side):
                self.arrived(
                    self.second, self.second_sem, (core, lax.rem(self.own_second + k, side))
                )
            for k in range(side):
                self.arrived(self.second, self.second_sem, (1 - core, k))
            halves = []
            for half in range(2):
                values = [self.second[half, k] for k in range(side)]
                while len(values) > 1:
                    values = [p + q for p, q in zip(values[::2], values[1::2])]
                halves.append(values[0])
            return jnp.concatenate(halves, axis=0)

        def drain(self):
            for k in range(1, side):
                for half in range(2):
                    self.first_send(half, k).wait_send()
                    self.second_send(half, k).wait_send()
            self.first_partner().wait_send()
            self.second_partner().wait_send()

    channels, taken = [], 0
    for tiles in CHANNELS:
        channels.append([])
        for _ in tiles:
            channels[-1].append(Channel(channel_refs[taken : taken + 6]))
            taken += 6

    def drain(app):
        @pl.when(me < count - 1)
        def _():
            forward(app).wait_send()

        @pl.when(me > 0)
        def _():
            backward(app).wait_send()

        for channel in channels[app]:
            channel.drain()

    def wide(refs, group):
        return jnp.concatenate(
            [
                jnp.concatenate([ref[group * REACH + k + shift] for ref, shift in refs], axis=0)
                for k in range(REACH)
            ],
            axis=1,
        )

    def wide_row(ref, group):
        return jnp.concatenate(
            [ref[group * REACH + k : group * REACH + k + 1, :] for k in range(REACH)], axis=1
        )

    for b in range(blocks + REACH):
        product[b, SLOTS] = jnp.zeros((MODES, WIDTH), jnp.float32)
    for copy in loads:
        copy.wait()
    acc = jnp.zeros((MODES, MODES), jnp.float32)
    for g in range(groups):
        left = wide([(ext0, REACH)], g)
        acc = acc + mm3(left * wide_row(mass, g), left, True)
    channels[0][0].store(pack32(acc))
    table_load.wait()
    for b in range(blocks):
        for d in range(1, REACH + 1):
            slot = SLOTS
            for s in range(SLOTS):
                slot = jnp.where(offsets[s, b] == d, s, slot)
            slot_of[b, d - 1] = slot
    for b in range(blocks, blocks + REACH):
        for d in range(REACH):
            slot_of[b, d] = SLOTS

    def ready(g):
        for copy in matrix_loads[g]:
            copy.wait()
        for b in range(g * REACH, (g + 1) * REACH):
            whole = jnp.concatenate([diag[b]] + [coupling[b, s] for s in range(SLOTS)], axis=1)
            high[b], low[b] = split(whole)

    ready(0)
    for b in range(REACH):
        own_products(ext0, b)
    pl.semaphore_wait(barrier, len(greeted))
    send_forward(0)
    send_backward(0)
    channels[0][0].start()
    channels[0][1].store(pack32(rest_of_product(0, ready)))
    channels[0][1].start()
    identity = eye(WIDTH)
    for b in range(blocks):
        inverse_diag[b : b + 1, :] = 1.0 / jnp.sum(diag[b] * identity, axis=0, keepdims=True)
    channels[0][0].middle()
    channels[0][1].middle()
    factor = first_factor(unpack32(channels[0][0].finish()))
    block = unpack32(channels[0][1].finish())
    projected = mm_nt(mm(factor, block, HIGHEST), factor, HIGHEST)
    projected = 0.5 * (projected + projected.T)
    coefficients = factor
    basis, stiff_basis = [(ext0, REACH)], [(stiff_new, 0)]
    previous = None

    for step in range(1, ITERS + 1):
        ext = exts[step]
        order = coefficients.shape[1]
        later = jnp.where(lanes((MODES, order)) < MODES, 0.0, coefficients)
        moving = previous is not None
        both = jnp.concatenate([coefficients, later], axis=0) if moving else coefficients
        n = MODES * (3 if moving else 2)
        stiff_acc = jnp.zeros((MODES, n - MODES), jnp.float32)
        mass_acc = jnp.zeros((MODES, n), jnp.float32)
        for g in (groups - 1, 0, *range(1, groups - 1)):
            new = mm3(both, wide(basis, g))
            stiff = mm3(both, wide(stiff_basis, g))
            masses = wide_row(mass, g)
            residual = stiff[:MODES] - mm3(projected, new[:MODES] * masses)
            residual = residual * wide_row(inverse_diag, g)
            for k in range(REACH):
                b = g * REACH + k
                cut = slice(k * WIDTH, (k + 1) * WIDTH)
                modes[b] = new[:MODES, cut]
                stiff_modes[b] = stiff[:MODES, cut]
                ext[b + REACH] = residual[:, cut]
                if moving:
                    direction[b] = new[MODES:, cut]
                    stiff_direction[b] = stiff[MODES:, cut]
            right = [new[:MODES], residual] + ([new[MODES:]] if moving else [])
            mass_acc = mass_acc + mm3(residual * masses, jnp.concatenate(right, axis=0), True)
            stiff_acc = stiff_acc + mm3(residual, stiff, True)
            if g == 0:
                for b in range(REACH):
                    own_products(ext, b)
                send_forward(step)
                send_backward(step)
        mass_sum, stiff_sum, late_sum = channels[step]
        mass_sum.store(pack96(mass_acc) if moving else pack64(mass_acc))
        stiff_sum.store(pack64(stiff_acc) if moving else pack32(stiff_acc))
        mass_sum.start()
        stiff_sum.start()
        late_sum.store(pack32(rest_of_product(step, lambda g: None)))
        late_sum.start()
        basis = [(modes, 0), (ext, REACH)] + ([(direction, 0)] if moving else [])
        stiff_basis = [(stiff_modes, 0), (stiff_new, 0)] + ([(stiff_direction, 0)] if moving else [])
        shape = (MODES, n)
        lane = lanes(shape)
        unit = jnp.where(lane == sublanes(shape), 1.0, 0.0)
        placed = mm(0.5 * projected, unit, HIGHEST)
        third = []
        if moving:
            zero = jnp.zeros((MODES, order), jnp.float32)
            spread_rows = jnp.concatenate([coefficients, zero, later], axis=0)
            third = [
                [
                    mm_nt(mm(later, old, HIGHEST), spread_rows, HIGHEST)
                    * jnp.where(lane < 2 * MODES, 1.0, 0.5)
                ]
                for old in previous
            ]
        else:
            third = [[], []]
        drain(step - 1)
        mass_sum.middle()
        stiff_sum.middle()
        late_sum.middle()
        early_mass = mass_sum.finish()
        early_mass = unpack96(early_mass) if moving else unpack64(early_mass)
        half = jnp.where((lane >= MODES) & (lane < 2 * MODES), 0.5, 1.0)
        gram_mass = jnp.concatenate([0.5 * unit, early_mass * half] + third[1], axis=0)
        gram_mass = gram_mass + gram_mass.T
        arrived = []

        def collect(arrived=arrived):
            arrived.append(stiff_sum.finish())
            arrived.append(late_sum.finish())

        factor = next_factor(gram_mass, collect if moving else lambda: None)
        if not moving:
            collect()
        early_stiff = unpack64(arrived[0]) if moving else unpack32(arrived[0])
        block_lane = lanes((8, WIDTH))
        here = (block_lane >= MODES) & (block_lane < 2 * MODES)
        turned = [arrived[1] if k == 1 else pltpu.roll(arrived[1], (1 - k) % 4 * MODES, 1) for k in range(4)]
        block = jnp.concatenate([jnp.where(here, 0.5 * t, 0.0) for t in turned], axis=0)[:, :n]
        empty = jnp.zeros((MODES, MODES), jnp.float32)
        pieces = [early_stiff[:, :MODES], empty] + ([early_stiff[:, MODES:]] if moving else [])
        gram_stiff = jnp.concatenate([placed, jnp.concatenate(pieces, axis=1) + block] + third[0], axis=0)
        gram_stiff = gram_stiff + gram_stiff.T
        reduced = mm_nt(mm(factor, gram_stiff, HIGHEST), factor, HIGHEST)
        coefficients, projected = ritz_rows(reduced, factor)
        previous = [gram_stiff, gram_mass]

    for g in range(groups):
        new = mm3(coefficients, wide(basis, g))
        stiff = mm3(coefficients, wide(stiff_basis, g))
        squares = jnp.sum(new * new, axis=0, keepdims=True)
        energy = jnp.sum(new * stiff, axis=0, keepdims=True)
        for k in range(REACH):
            cut = slice(k * WIDTH, (k + 1) * WIDTH)
            b = g * REACH + k
            out[0, b : b + 1, :] = squares[:, cut]
            out[1, b : b + 1, :] = energy[:, cut]
    drain(ITERS)


def solution(mesh):
    count = mesh.shape["row"]

    def local(diag_blocks, coupling, offsets, mass, initial_modes):
        blocks = diag_blocks.shape[0]
        apps = ITERS + 1
        side = TORUS[1]
        cores = TORUS[2]
        f32 = jnp.float32
        dma = pltpu.SemaphoreType.DMA
        vector = pltpu.VMEM((blocks, MODES, WIDTH), f32)
        extended = pltpu.VMEM((blocks + REACH, MODES, WIDTH), f32)
        halo = pltpu.VMEM((apps, REACH, MODES, WIDTH), f32)
        channel_shapes = []
        for tiles in CHANNELS:
            for tile in tiles:
                rows = 4 * tile
                channel_shapes += [
                    pltpu.VMEM((2, rows, WIDTH), f32),
                    pltpu.VMEM((side * cores, rows, WIDTH), f32),
                    pltpu.VMEM((2, side, rows, WIDTH), f32),
                    dma((2, 2, side)),
                    dma((side * cores,)),
                    dma((2, side)),
                ]
        sums = pl.pallas_call(
            lambda *refs: solve_kernel((count, blocks), *refs),
            out_shape=jax.ShapeDtypeStruct((2, blocks, WIDTH), f32),
            in_specs=[
                pl.BlockSpec(memory_space=pltpu.HBM),
                pl.BlockSpec(memory_space=pltpu.HBM),
                pl.BlockSpec(memory_space=pltpu.HBM),
                pl.BlockSpec(memory_space=pltpu.HBM),
                pl.BlockSpec(memory_space=pltpu.HBM),
            ],
            out_specs=pl.BlockSpec(memory_space=pltpu.VMEM),
            scratch_shapes=[
                pltpu.VMEM((blocks, WIDTH, WIDTH), f32),
                pltpu.VMEM((blocks, SLOTS, WIDTH, WIDTH), f32),
                pltpu.VMEM((blocks, WIDTH, (SLOTS + 1) * WIDTH), jnp.bfloat16),
                pltpu.VMEM((blocks, WIDTH, (SLOTS + 1) * WIDTH), jnp.bfloat16),
                pltpu.VMEM((blocks, WIDTH), f32),
                pltpu.SMEM((SLOTS, blocks), jnp.int32),
                pltpu.SMEM((blocks + REACH, REACH), jnp.int32),
                pltpu.VMEM((blocks, WIDTH), f32),
                pltpu.VMEM((blocks + REACH, SLOTS + 1, MODES, WIDTH), f32),
                extended,
                extended,
                extended,
                extended,
                vector,
                vector,
                vector,
                vector,
                vector,
                halo,
                halo,
                halo,
                dma((blocks + 2,)),
                dma((2, blocks // REACH)),
                dma((apps, 2)),
                dma((apps, 2)),
                *channel_shapes,
            ],
            compiler_params=pltpu.CompilerParams(
                collective_id=0, has_side_effects=True, vmem_limit_bytes=56 << 20
            ),
            name="lobpcg",
        )(diag_blocks, coupling, offsets.T, mass.reshape(blocks, WIDTH), initial_modes)
        weight = count * blocks * WIDTH / MODES
        return weight * mass * sums[0].reshape(-1), weight * sums[1].reshape(-1)

    spec = ("sub", "row")
    return jax.shard_map(
        local,
        mesh=mesh,
        in_specs=(
            P(spec, None, None),
            P(spec, None, None, None),
            P(spec, None),
            P(spec),
            P(None, spec),
        ),
        out_specs=(P(spec), P(spec)),
        check_vma=False,
    )
```

```python
import jax
import jax.numpy as jnp
from jax import lax
from jax.experimental import pallas as pl
from jax.experimental.pallas import tpu as pltpu
from jax.sharding import PartitionSpec as P

MODES = 32
REACH = 4
SLOTS = 3
ITERS = 3
PURIFY = 28
WIDTH = 128
TORUS = (8, 8, 2)
MESH = pl.DeviceIdType.MESH
CHANNELS = ((1, 1), (2, 1, 1), (3, 2, 1), (3, 2, 1))

HIGHEST = lax.Precision.HIGHEST


def mm(a, b, precision):
    return lax.dot_general(
        a, b, (((1,), (0,)), ((), ())), precision=precision, preferred_element_type=jnp.float32
    )


def mm_nt(a, b, precision):
    return lax.dot_general(
        a, b, (((1,), (1,)), ((), ())), precision=precision, preferred_element_type=jnp.float32
    )


def split(value):
    high = value.astype(jnp.bfloat16)
    return high, (value - high.astype(jnp.float32)).astype(jnp.bfloat16)


def mm3(a, b, transposed=False):
    contract = (((1,), (1 if transposed else 0,)), ((), ()))
    a_high, a_low = split(a)
    b_high, b_low = b if isinstance(b, tuple) else split(b)
    rows = a.shape[0]
    top = lax.dot_general(
        jnp.concatenate([a_high, a_low], axis=0),
        b_high,
        contract,
        preferred_element_type=jnp.float32,
    )
    rest = lax.dot_general(a_high, b_low, contract, preferred_element_type=jnp.float32)
    return (top[:rows] + rest) + top[rows:]


def lanes(shape):
    return lax.broadcasted_iota(jnp.int32, shape, 1)


def sublanes(shape):
    return lax.broadcasted_iota(jnp.int32, shape, 0)


def eye(n):
    return (sublanes((n, n)) == lanes((n, n))).astype(jnp.float32)


def total(x):
    return jnp.sum(jnp.sum(x, axis=0, keepdims=True), axis=1, keepdims=True)


def inverse_factor(table, first):
    rows, cols = table.shape
    index = sublanes((8, cols))
    lane = lanes((1, cols))
    done = []
    below = table
    for start in range(0, rows, 8):
        at = first + start
        top, below = below[:8], below[8:]
        parts = [top] + ([below] if below.shape[0] else [])
        columns = [
            [jnp.broadcast_to(part[:, at + k : at + k + 1], part.shape) for part in parts]
            for k in range(8)
        ]
        panel = (lane >= at) & (lane < at + 8)
        parts = [jnp.where(panel, 0.0, part) for part in parts]
        for k in range(0, 8, 2):
            one, two = columns[k], columns[k + 1]
            a, c = one[0][k : k + 1, :], two[0][k + 1 : k + 2, :]
            b = one[0][k + 1 : k + 2, :]
            scale = lax.rsqrt(a)
            rest = lax.rsqrt(a * c - b * b)
            scale_two = a * scale * rest
            cross = b * scale * rest
            row = (parts[0][k : k + 1, :] + jnp.where(lane == at + k, 1.0, 0.0)) * scale
            row_two = (
                parts[0][k + 1 : k + 2, :] + jnp.where(lane == at + k + 1, 1.0, 0.0)
            ) * scale_two - cross * (parts[0][k : k + 1, :] + jnp.where(lane == at + k, 1.0, 0.0))
            factors = [column * scale for column in one]
            factors_two = [q * scale_two - p * cross for p, q in zip(one, two)]
            factors[0] = jnp.where(index > k + 1, factors[0], 0.0)
            factors_two[0] = jnp.where(index > k + 1, factors_two[0], 0.0)
            parts = [
                part - f * row - g * row_two for part, f, g in zip(parts, factors, factors_two)
            ]
            parts[0] = jnp.where(index == k, row, jnp.where(index == k + 1, row_two, parts[0]))
            for m in range(k + 2, 8):
                entry = columns[m][0][k : k + 1, :] * scale
                entry_two = columns[m][0][k + 1 : k + 2, :] * scale_two - cross * columns[m][0][k : k + 1, :]
                columns[m] = [
                    c_ - f * entry - g * entry_two
                    for c_, f, g in zip(columns[m], factors, factors_two)
                ]
        done.append(parts[0])
        below = parts[-1]
    result = jnp.concatenate(done, axis=0)
    shape = (rows, cols)
    return jnp.where(lanes(shape) <= sublanes(shape) + first, result, 0.0)


def purify(matrix):
    n = matrix.shape[0]
    identity = eye(n)
    diagonal = jnp.sum(matrix * identity, axis=0, keepdims=True)
    radius = jnp.sum(jnp.abs(matrix), axis=0, keepdims=True) - jnp.abs(diagonal)
    center = jnp.sum(diagonal, axis=1, keepdims=True) / n
    highest = jnp.max(diagonal + radius, axis=1, keepdims=True)
    lowest = jnp.min(diagonal - radius, axis=1, keepdims=True)
    factor = jnp.minimum(
        MODES / jnp.maximum(highest - center, 1e-6), (n - MODES) / jnp.maximum(center - lowest, 1e-6)
    )
    initial = factor / n * (center * identity - matrix) + MODES / n * identity
    edge = jnp.zeros((n, WIDTH - n), jnp.float32)
    initial = jnp.concatenate([initial, edge], axis=1)
    identity = jnp.where(lanes((n, WIDTH)) == sublanes((n, WIDTH)), 1.0, 0.0)
    fill = jnp.zeros((WIDTH - n, WIDTH), jnp.bfloat16)
    empty = jnp.zeros((WIDTH, WIDTH), jnp.bfloat16)

    def step(index, density):
        high, low = [jnp.concatenate([part, fill], axis=0) for part in split(density)]
        weights = jnp.concatenate(
            [jnp.concatenate([high, low], axis=1), jnp.concatenate([high, empty], axis=1)], axis=0
        )

        def times_density(value):
            both = lax.dot_general(
                jnp.concatenate(split(value), axis=1),
                weights,
                (((1,), (0,)), ((), ())),
                preferred_element_type=jnp.float32,
            )
            return both[:, :WIDTH] + both[:, WIDTH:]

        square = times_density(density)
        cube = times_density(square)
        denominator = total((density - square) * identity)
        numerator = total(square * (identity - density))
        safe = jnp.where(jnp.abs(denominator) > 1e-12, denominator, 1.0)
        ratio = jnp.clip(numerator / safe, 0.0, 1.0)
        up = ratio >= 0.5
        scale = 1.0 / jnp.maximum(jnp.where(up, ratio, 1.0 - ratio), 0.5)
        first = jnp.where(up, 0.0, (1.0 - 2.0 * ratio) * scale)
        second = (1.0 + ratio) * scale
        return first * density + second * square - scale * cube

    return lax.fori_loop(0, PURIFY, step, initial)[:MODES, :n]


def pack32(block):
    return jnp.concatenate([block[8 * k : 8 * k + 8] for k in range(4)], axis=1)


def unpack32(tile):
    return jnp.concatenate([tile[:, MODES * k : MODES * (k + 1)] for k in range(4)], axis=0)


def pack64(block):
    return jnp.concatenate([block[:16], block[16:]], axis=1)


def unpack64(tile):
    return jnp.concatenate([tile[:, : 2 * MODES], tile[:, 2 * MODES :]], axis=0)


def pack96(block):
    last = [block[24:, MODES * k : MODES * (k + 1)] for k in range(3)]
    return jnp.concatenate([block[:24], jnp.concatenate(last, axis=0)], axis=1)


def unpack96(tile):
    last = [tile[8 * k : 8 * k + 8, 3 * MODES :] for k in range(3)]
    return jnp.concatenate([tile[:, : 3 * MODES], jnp.concatenate(last, axis=1)], axis=0)


def first_factor(gram_mass):
    return inverse_factor(0.5 * (gram_mass + gram_mass.T), 0)


def next_factor(gram_mass):
    n = gram_mass.shape[0]
    rest = n - MODES
    side = gram_mass[:, :MODES]
    side = jnp.where(sublanes((n, MODES)) < MODES, 0.0, side)
    lower = gram_mass[MODES:, :]
    schur = lower - mm_nt(side[MODES:], side, HIGHEST)
    bottom = inverse_factor(jnp.where(lanes((rest, n)) < MODES, -lower, schur), MODES)
    shape = (MODES, n)
    unit = jnp.where(lanes(shape) == sublanes(shape), 1.0, 0.0)
    return jnp.concatenate([unit, bottom], axis=0)


def ritz_rows(reduced, factor):
    rows = purify(reduced)
    change = inverse_factor(mm_nt(rows, rows, HIGHEST), 0)
    coefficients = mm(rows, factor, HIGHEST)
    projected = mm_nt(mm(rows, reduced, HIGHEST), rows, HIGHEST)
    coefficients = mm(change, coefficients, HIGHEST)
    projected = mm_nt(mm(change, projected, HIGHEST), change, HIGHEST)
    return coefficients, projected


def solve_kernel(
    sizes,
    diag_hbm,
    coupling_hbm,
    offsets_hbm,
    mass_hbm,
    initial_hbm,
    out,
    diag,
    coupling,
    high,
    low,
    mass,
    offsets,
    slot_of,
    inverse_diag,
    product,
    ext0,
    ext1,
    ext2,
    ext3,
    stiff_new,
    modes,
    stiff_modes,
    direction,
    stiff_direction,
    edge,
    landing,
    returned,
    load_sem,
    matrix_sem,
    halo_send,
    halo_recv,
    *channel_refs,
):
    count, blocks = sizes
    ny, nx, cores = TORUS
    side = nx
    me = lax.axis_index("row")
    core = lax.rem(me, cores)
    x = lax.rem(lax.div(me, cores), nx)
    y = lax.div(me, cores * nx)
    partner = me + 1 - 2 * core
    exts = (ext0, ext1, ext2, ext3)
    groups = blocks // REACH

    table_load = pltpu.make_async_copy(offsets_hbm, offsets, load_sem.at[blocks + 1])
    loads = [pltpu.make_async_copy(mass_hbm, mass, load_sem.at[blocks])]
    loads += [
        pltpu.make_async_copy(
            initial_hbm.at[:, pl.ds(b * WIDTH, WIDTH)], ext0.at[b + REACH], load_sem.at[b]
        )
        for b in range(blocks)
    ]
    matrix_loads = [
        [
            pltpu.make_async_copy(
                ref.at[pl.ds(g * REACH, REACH)], out.at[pl.ds(g * REACH, REACH)], matrix_sem.at[i, g]
            )
            for i, (ref, out) in enumerate([(diag_hbm, diag), (coupling_hbm, coupling)])
        ]
        for g in range(groups)
    ]
    table_load.start()
    for copy in loads:
        copy.start()
    for pair in matrix_loads:
        for copy in pair:
            copy.start()

    farthest = sorted(range(1, side), key=lambda k: -min(k, side - k))
    x_at = [lax.rem(x + k, nx) for k in range(side)]
    y_at = [lax.rem(y + k, ny) for k in range(side)]

    def device(px, py, pcore):
        return {"row": (py * nx + px) * cores + pcore}

    barrier = pltpu.get_barrier_semaphore()
    greeted = [{"row": partner}, {"row": lax.rem(me + 1, count)}, {"row": lax.rem(me + count - 1, count)}]
    for k in range(1, side):
        for pcore in range(cores):
            greeted += [device(x_at[k], y, pcore), device(x, y_at[k], pcore)]
    for other in greeted:
        pl.semaphore_signal(barrier, inc=1, device_id=other, device_id_type=MESH)

    def send(source, target, send_sem, recv_sem, other):
        return pltpu.make_async_remote_copy(
            src_ref=source,
            dst_ref=target,
            send_sem=send_sem,
            recv_sem=recv_sem,
            device_id=other,
            device_id_type=MESH,
        )

    def forward(app):
        return send(
            exts[app].at[pl.ds(blocks, REACH)],
            landing.at[app],
            halo_send.at[app, 0],
            halo_recv.at[app, 0],
            {"row": me + 1},
        )

    def backward(app):
        return send(
            edge.at[app],
            returned.at[app],
            halo_send.at[app, 1],
            halo_recv.at[app, 1],
            {"row": me - 1},
        )

    def own_products(ext, b):
        out = mm3(ext[b + REACH], (high[b], low[b]))
        stiff_new[b] = out[:, :WIDTH]
        for s in range(SLOTS):
            product[b, s] = out[:, (s + 1) * WIDTH : (s + 2) * WIDTH]

    def other_products(ext, b):
        taken = jnp.concatenate([ext[b + REACH - offsets[s, b]] for s in range(SLOTS)], axis=1)
        spread = [product[b + d, slot_of[b + d, d - 1]] for d in range(1, REACH + 1)]
        spread = (spread[0] + spread[1]) + (spread[2] + spread[3])
        out = mm3(taken, (high[b, :, WIDTH:], low[b, :, WIDTH:]), True)
        stiff_new[b] = stiff_new[b] + out + spread

    def send_forward(app):
        @pl.when(me < count - 1)
        def _():
            forward(app).start()

    def send_backward(app):
        for e in range(REACH):
            out = jnp.zeros((MODES, WIDTH), jnp.float32)
            for b in range(e + 1):
                out = out + product[b, slot_of[b, b - e + REACH - 1]]
            edge[app, e] = out

        @pl.when(me > 0)
        def _():
            backward(app).start()

    def late_part(app, g):
        return mm3(wide([(exts[app], REACH)], g), wide([(stiff_new, 0)], g), True)

    def rest_of_product(app, ready):
        ext = exts[app]
        for g in range(1, groups):
            ready(g)
            for b in range(g * REACH, (g + 1) * REACH):
                own_products(ext, b)
        for b in range(REACH, blocks):
            other_products(ext, b)
        acc = late_part(app, 1)
        for g in range(2, groups - 1):
            acc = acc + late_part(app, g)

        @pl.when(me > 0)
        def _():
            forward(app).wait_recv()
            ext[0:REACH] = landing[app]

        @pl.when(me == 0)
        def _():
            ext[0:REACH] = jnp.zeros((REACH, MODES, WIDTH), jnp.float32)

        for b in range(REACH):
            other_products(ext, b)
        acc = acc + late_part(app, 0)

        @pl.when(me < count - 1)
        def _():
            backward(app).wait_recv()
            for k in range(REACH):
                b = blocks - REACH + k
                stiff_new[b] = stiff_new[b] + returned[app, k]

        return acc + late_part(app, groups - 1)

    class Channel:
        def __init__(self, refs):
            (self.part, self.first, self.second, self.sends, self.first_sem, self.second_sem) = refs
            self.own_first = (x * (1 - core) + y * core) * cores + core
            self.own_second = y * (1 - core) + x * core

        def first_send(self, half, k):
            if half == 0:
                slot, target = x * cores + core, device(x_at[k], y, 0)
            else:
                slot, target = y * cores + core, device(x, y_at[k], 1)
            return send(
                self.part.at[half],
                self.first.at[slot],
                self.sends.at[0, half, k],
                self.first_sem.at[slot],
                target,
            )

        def first_partner(self):
            half = 1 - core
            slot = (x * core + y * half) * cores + core
            return send(
                self.part.at[half],
                self.first.at[slot],
                self.sends.at[0, half, 0],
                self.first_sem.at[slot],
                {"row": partner},
            )

        def second_send(self, pcore, k):
            where = self.own_second
            px = x * (1 - core) + x_at[k] * core
            py = y_at[k] * (1 - core) + y * core
            return send(
                self.second.at[core, where],
                self.second.at[core, where],
                self.sends.at[1, pcore, k],
                self.second_sem.at[core, where],
                device(px, py, pcore),
            )

        def second_partner(self):
            where = self.own_second
            return send(
                self.second.at[core, where],
                self.second.at[core, where],
                self.sends.at[1, 1 - core, 0],
                self.second_sem.at[core, where],
                {"row": partner},
            )

        def arrived(self, buffer, sem, index):
            send(
                buffer.at[index], buffer.at[index], self.sends.at[0, 0, 0], sem.at[index],
                {"row": partner},
            ).wait_recv()

        def store(self, packed):
            rows = packed.shape[0] // 2
            self.part[0] = packed[:rows]
            self.part[1] = packed[rows:]

        def start(self):
            self.first[self.own_first] = self.part[core]
            for k in farthest:
                for half in range(2):
                    self.first_send(half, k).start()
            self.first_partner().start()

        def middle(self):
            slots = side * cores
            for k in range(1, slots):
                self.arrived(self.first, self.first_sem, lax.rem(self.own_first + k, slots))
            values = [self.first[k] for k in range(slots)]
            while len(values) > 1:
                values = [p + q for p, q in zip(values[::2], values[1::2])]
            self.second[core, self.own_second] = values[0]
            for k in farthest:
                for pcore in range(cores):
                    self.second_send(pcore, k).start()
            self.second_partner().start()

        def finish(self):
            for k in range(1, side):
                self.arrived(
                    self.second, self.second_sem, (core, lax.rem(self.own_second + k, side))
                )
            for k in range(side):
                self.arrived(self.second, self.second_sem, (1 - core, k))
            halves = []
            for half in range(2):
                values = [self.second[half, k] for k in range(side)]
                while len(values) > 1:
                    values = [p + q for p, q in zip(values[::2], values[1::2])]
                halves.append(values[0])
            return jnp.concatenate(halves, axis=0)

        def drain(self):
            for k in range(1, side):
                for half in range(2):
                    self.first_send(half, k).wait_send()
                    self.second_send(half, k).wait_send()
            self.first_partner().wait_send()
            self.second_partner().wait_send()

    channels, taken = [], 0
    for tiles in CHANNELS:
        channels.append([])
        for _ in tiles:
            channels[-1].append(Channel(channel_refs[taken : taken + 6]))
            taken += 6

    def drain(app):
        @pl.when(me < count - 1)
        def _():
            forward(app).wait_send()

        @pl.when(me > 0)
        def _():
            backward(app).wait_send()

        for channel in channels[app]:
            channel.drain()

    def wide(refs, group):
        return jnp.concatenate(
            [
                jnp.concatenate([ref[group * REACH + k + shift] for ref, shift in refs], axis=0)
                for k in range(REACH)
            ],
            axis=1,
        )

    def wide_row(ref, group):
        return jnp.concatenate(
            [ref[group * REACH + k : group * REACH + k + 1, :] for k in range(REACH)], axis=1
        )

    for b in range(blocks + REACH):
        product[b, SLOTS] = jnp.zeros((MODES, WIDTH), jnp.float32)
    for copy in loads:
        copy.wait()
    acc = jnp.zeros((MODES, MODES), jnp.float32)
    for g in range(groups):
        left = wide([(ext0, REACH)], g)
        acc = acc + mm3(left * wide_row(mass, g), left, True)
    channels[0][0].store(pack32(acc))
    table_load.wait()
    for b in range(blocks):
        for d in range(1, REACH + 1):
            slot = SLOTS
            for s in range(SLOTS):
                slot = jnp.where(offsets[s, b] == d, s, slot)
            slot_of[b, d - 1] = slot
    for b in range(blocks, blocks + REACH):
        for d in range(REACH):
            slot_of[b, d] = SLOTS

    def ready(g):
        for copy in matrix_loads[g]:
            copy.wait()
        for b in range(g * REACH, (g + 1) * REACH):
            whole = jnp.concatenate([diag[b]] + [coupling[b, s] for s in range(SLOTS)], axis=1)
            high[b], low[b] = split(whole)

    ready(0)
    for b in range(REACH):
        own_products(ext0, b)
    pl.semaphore_wait(barrier, len(greeted))
    send_forward(0)
    send_backward(0)
    channels[0][0].start()
    channels[0][1].store(pack32(rest_of_product(0, ready)))
    channels[0][1].start()
    identity = eye(WIDTH)
    for b in range(blocks):
        inverse_diag[b : b + 1, :] = 1.0 / jnp.sum(diag[b] * identity, axis=0, keepdims=True)
    channels[0][0].middle()
    channels[0][1].middle()
    factor = first_factor(unpack32(channels[0][0].finish()))
    block = unpack32(channels[0][1].finish())
    projected = mm_nt(mm(factor, block, HIGHEST), factor, HIGHEST)
    projected = 0.5 * (projected + projected.T)
    coefficients = factor
    basis, stiff_basis = [(ext0, REACH)], [(stiff_new, 0)]
    previous = None

    for step in range(1, ITERS + 1):
        ext = exts[step]
        order = coefficients.shape[1]
        later = jnp.where(lanes((MODES, order)) < MODES, 0.0, coefficients)
        moving = previous is not None
        both = jnp.concatenate([coefficients, later], axis=0) if moving else coefficients
        n = MODES * (3 if moving else 2)
        stiff_acc = jnp.zeros((MODES, n - MODES), jnp.float32)
        mass_acc = jnp.zeros((MODES, n), jnp.float32)
        for g in (groups - 1, 0, *range(1, groups - 1)):
            new = mm3(both, wide(basis, g))
            stiff = mm3(both, wide(stiff_basis, g))
            masses = wide_row(mass, g)
            residual = stiff[:MODES] - mm3(projected, new[:MODES] * masses)
            residual = residual * wide_row(inverse_diag, g)
            for k in range(REACH):
                b = g * REACH + k
                cut = slice(k * WIDTH, (k + 1) * WIDTH)
                modes[b] = new[:MODES, cut]
                stiff_modes[b] = stiff[:MODES, cut]
                ext[b + REACH] = residual[:, cut]
                if moving:
                    direction[b] = new[MODES:, cut]
                    stiff_direction[b] = stiff[MODES:, cut]
            right = [new[:MODES], residual] + ([new[MODES:]] if moving else [])
            mass_acc = mass_acc + mm3(residual * masses, jnp.concatenate(right, axis=0), True)
            stiff_acc = stiff_acc + mm3(residual, stiff, True)
            if g == 0:
                for b in range(REACH):
                    own_products(ext, b)
                send_forward(step)
                send_backward(step)
        mass_sum, stiff_sum, late_sum = channels[step]
        mass_sum.store(pack96(mass_acc) if moving else pack64(mass_acc))
        stiff_sum.store(pack64(stiff_acc) if moving else pack32(stiff_acc))
        mass_sum.start()
        stiff_sum.start()
        late_sum.store(pack32(rest_of_product(step, lambda g: None)))
        late_sum.start()
        basis = [(modes, 0), (ext, REACH)] + ([(direction, 0)] if moving else [])
        stiff_basis = [(stiff_modes, 0), (stiff_new, 0)] + ([(stiff_direction, 0)] if moving else [])
        shape = (MODES, n)
        lane = lanes(shape)
        unit = jnp.where(lane == sublanes(shape), 1.0, 0.0)
        placed = mm(0.5 * projected, unit, HIGHEST)
        third = []
        if moving:
            zero = jnp.zeros((MODES, order), jnp.float32)
            spread_rows = jnp.concatenate([coefficients, zero, later], axis=0)
            third = [
                [
                    mm_nt(mm(later, old, HIGHEST), spread_rows, HIGHEST)
                    * jnp.where(lane < 2 * MODES, 1.0, 0.5)
                ]
                for old in previous
            ]
        else:
            third = [[], []]
        drain(step - 1)
        mass_sum.middle()
        stiff_sum.middle()
        late_sum.middle()
        early_mass = mass_sum.finish()
        early_mass = unpack96(early_mass) if moving else unpack64(early_mass)
        half = jnp.where((lane >= MODES) & (lane < 2 * MODES), 0.5, 1.0)
        gram_mass = jnp.concatenate([0.5 * unit, early_mass * half] + third[1], axis=0)
        gram_mass = gram_mass + gram_mass.T
        factor = next_factor(gram_mass)
        middle = factor[:, MODES : 2 * MODES]
        early_stiff = stiff_sum.finish()
        early_stiff = unpack64(early_stiff) if moving else unpack32(early_stiff)
        empty = jnp.zeros((MODES, MODES), jnp.float32)
        pieces = [early_stiff[:, :MODES], empty] + ([early_stiff[:, MODES:]] if moving else [])
        rest = jnp.concatenate([placed, jnp.concatenate(pieces, axis=1)] + third[0], axis=0)
        rest = rest + rest.T
        known = mm_nt(mm(factor, rest, HIGHEST), factor, HIGHEST)
        tile = late_sum.finish()
        block = unpack32(tile)
        reduced = known + mm_nt(mm(middle, block, HIGHEST), middle, HIGHEST)
        coefficients, projected = ritz_rows(reduced, factor)
        if step < ITERS:
            block_lane = lanes((8, WIDTH))
            here = (block_lane >= MODES) & (block_lane < 2 * MODES)
            turned = [tile if k == 1 else pltpu.roll(tile, (1 - k) % 4 * MODES, 1) for k in range(4)]
            inner = jnp.concatenate([jnp.where(here, t, 0.0) for t in turned], axis=0)[:, :n]
            empty = jnp.zeros((MODES, n), jnp.float32)
            inner = jnp.concatenate([empty, inner] + [empty] * (n // MODES - 2), axis=0)
            previous = [rest + inner, gram_mass]

    for g in range(groups):
        new = mm3(coefficients, wide(basis, g))
        stiff = mm3(coefficients, wide(stiff_basis, g))
        squares = jnp.sum(new * new, axis=0, keepdims=True)
        energy = jnp.sum(new * stiff, axis=0, keepdims=True)
        for k in range(REACH):
            cut = slice(k * WIDTH, (k + 1) * WIDTH)
            b = g * REACH + k
            out[0, b : b + 1, :] = squares[:, cut]
            out[1, b : b + 1, :] = energy[:, cut]
    drain(ITERS)


def solution(mesh):
    count = mesh.shape["row"]

    def local(diag_blocks, coupling, offsets, mass, initial_modes):
        blocks = diag_blocks.shape[0]
        apps = ITERS + 1
        side = TORUS[1]
        cores = TORUS[2]
        f32 = jnp.float32
        dma = pltpu.SemaphoreType.DMA
        vector = pltpu.VMEM((blocks, MODES, WIDTH), f32)
        extended = pltpu.VMEM((blocks + REACH, MODES, WIDTH), f32)
        halo = pltpu.VMEM((apps, REACH, MODES, WIDTH), f32)
        channel_shapes = []
        for tiles in CHANNELS:
            for tile in tiles:
                rows = 4 * tile
                channel_shapes += [
                    pltpu.VMEM((2, rows, WIDTH), f32),
                    pltpu.VMEM((side * cores, rows, WIDTH), f32),
                    pltpu.VMEM((2, side, rows, WIDTH), f32),
                    dma((2, 2, side)),
                    dma((side * cores,)),
                    dma((2, side)),
                ]
        sums = pl.pallas_call(
            lambda *refs: solve_kernel((count, blocks), *refs),
            out_shape=jax.ShapeDtypeStruct((2, blocks, WIDTH), f32),
            in_specs=[
                pl.BlockSpec(memory_space=pltpu.HBM),
                pl.BlockSpec(memory_space=pltpu.HBM),
                pl.BlockSpec(memory_space=pltpu.HBM),
                pl.BlockSpec(memory_space=pltpu.HBM),
                pl.BlockSpec(memory_space=pltpu.HBM),
            ],
            out_specs=pl.BlockSpec(memory_space=pltpu.VMEM),
            scratch_shapes=[
                pltpu.VMEM((blocks, WIDTH, WIDTH), f32),
                pltpu.VMEM((blocks, SLOTS, WIDTH, WIDTH), f32),
                pltpu.VMEM((blocks, WIDTH, (SLOTS + 1) * WIDTH), jnp.bfloat16),
                pltpu.VMEM((blocks, WIDTH, (SLOTS + 1) * WIDTH), jnp.bfloat16),
                pltpu.VMEM((blocks, WIDTH), f32),
                pltpu.SMEM((SLOTS, blocks), jnp.int32),
                pltpu.SMEM((blocks + REACH, REACH), jnp.int32),
                pltpu.VMEM((blocks, WIDTH), f32),
                pltpu.VMEM((blocks + REACH, SLOTS + 1, MODES, WIDTH), f32),
                extended,
                extended,
                extended,
                extended,
                vector,
                vector,
                vector,
                vector,
                vector,
                halo,
                halo,
                halo,
                dma((blocks + 2,)),
                dma((2, blocks // REACH)),
                dma((apps, 2)),
                dma((apps, 2)),
                *channel_shapes,
            ],
            compiler_params=pltpu.CompilerParams(
                collective_id=0, has_side_effects=True, vmem_limit_bytes=56 << 20
            ),
            name="lobpcg",
        )(diag_blocks, coupling, offsets.T, mass.reshape(blocks, WIDTH), initial_modes)
        weight = count * blocks * WIDTH / MODES
        return weight * mass * sums[0].reshape(-1), weight * sums[1].reshape(-1)

    spec = ("sub", "row")
    return jax.shard_map(
        local,
        mesh=mesh,
        in_specs=(
            P(spec, None, None),
            P(spec, None, None, None),
            P(spec, None),
            P(spec),
            P(None, spec),
        ),
        out_specs=(P(spec), P(spec)),
        check_vma=False,
    )
```

```python
import jax
import jax.numpy as jnp
from jax import lax
from jax.experimental import pallas as pl
from jax.experimental.pallas import tpu as pltpu
from jax.sharding import PartitionSpec as P

MODES = 32
REACH = 4
SLOTS = 3
ITERS = 3
PURIFY = 28
WIDTH = 128
TORUS = (8, 8, 2)
MESH = pl.DeviceIdType.MESH
CHANNELS = ((1, 1), (3, 1), (5, 1), (5, 1))

HIGHEST = lax.Precision.HIGHEST


def mm(a, b, precision):
    return lax.dot_general(
        a, b, (((1,), (0,)), ((), ())), precision=precision, preferred_element_type=jnp.float32
    )


def mm_nt(a, b, precision):
    return lax.dot_general(
        a, b, (((1,), (1,)), ((), ())), precision=precision, preferred_element_type=jnp.float32
    )


def split(value):
    high = value.astype(jnp.bfloat16)
    return high, (value - high.astype(jnp.float32)).astype(jnp.bfloat16)


def mm3(a, b, transposed=False):
    contract = (((1,), (1 if transposed else 0,)), ((), ()))
    a_high, a_low = split(a)
    b_high, b_low = b if isinstance(b, tuple) else split(b)
    rows = a.shape[0]
    top = lax.dot_general(
        jnp.concatenate([a_high, a_low], axis=0),
        b_high,
        contract,
        preferred_element_type=jnp.float32,
    )
    rest = lax.dot_general(a_high, b_low, contract, preferred_element_type=jnp.float32)
    return (top[:rows] + rest) + top[rows:]


def lanes(shape):
    return lax.broadcasted_iota(jnp.int32, shape, 1)


def sublanes(shape):
    return lax.broadcasted_iota(jnp.int32, shape, 0)


def eye(n):
    return (sublanes((n, n)) == lanes((n, n))).astype(jnp.float32)


def total(x):
    return jnp.sum(jnp.sum(x, axis=0, keepdims=True), axis=1, keepdims=True)


def inverse_factor(table, first):
    rows, cols = table.shape
    index = sublanes((8, cols))
    lane = lanes((1, cols))
    done = []
    below = table
    for start in range(0, rows, 8):
        at = first + start
        top, below = below[:8], below[8:]
        parts = [top] + ([below] if below.shape[0] else [])
        columns = [
            [jnp.broadcast_to(part[:, at + k : at + k + 1], part.shape) for part in parts]
            for k in range(8)
        ]
        panel = (lane >= at) & (lane < at + 8)
        parts = [jnp.where(panel, 0.0, part) for part in parts]
        for k in range(0, 8, 2):
            one, two = columns[k], columns[k + 1]
            a, c = one[0][k : k + 1, :], two[0][k + 1 : k + 2, :]
            b = one[0][k + 1 : k + 2, :]
            scale = lax.rsqrt(a)
            rest = lax.rsqrt(a * c - b * b)
            scale_two = a * scale * rest
            cross = b * scale * rest
            row = (parts[0][k : k + 1, :] + jnp.where(lane == at + k, 1.0, 0.0)) * scale
            row_two = (
                parts[0][k + 1 : k + 2, :] + jnp.where(lane == at + k + 1, 1.0, 0.0)
            ) * scale_two - cross * (parts[0][k : k + 1, :] + jnp.where(lane == at + k, 1.0, 0.0))
            factors = [column * scale for column in one]
            factors_two = [q * scale_two - p * cross for p, q in zip(one, two)]
            factors[0] = jnp.where(index > k + 1, factors[0], 0.0)
            factors_two[0] = jnp.where(index > k + 1, factors_two[0], 0.0)
            parts = [
                part - f * row - g * row_two for part, f, g in zip(parts, factors, factors_two)
            ]
            parts[0] = jnp.where(index == k, row, jnp.where(index == k + 1, row_two, parts[0]))
            for m in range(k + 2, 8):
                entry = columns[m][0][k : k + 1, :] * scale
                entry_two = columns[m][0][k + 1 : k + 2, :] * scale_two - cross * columns[m][0][k : k + 1, :]
                columns[m] = [
                    c_ - f * entry - g * entry_two
                    for c_, f, g in zip(columns[m], factors, factors_two)
                ]
        done.append(parts[0])
        below = parts[-1]
    result = jnp.concatenate(done, axis=0)
    shape = (rows, cols)
    return jnp.where(lanes(shape) <= sublanes(shape) + first, result, 0.0)


def purify(matrix):
    n = matrix.shape[0]
    identity = eye(n)
    diagonal = jnp.sum(matrix * identity, axis=0, keepdims=True)
    radius = jnp.sum(jnp.abs(matrix), axis=0, keepdims=True) - jnp.abs(diagonal)
    center = jnp.sum(diagonal, axis=1, keepdims=True) / n
    highest = jnp.max(diagonal + radius, axis=1, keepdims=True)
    lowest = jnp.min(diagonal - radius, axis=1, keepdims=True)
    factor = jnp.minimum(
        MODES / jnp.maximum(highest - center, 1e-6), (n - MODES) / jnp.maximum(center - lowest, 1e-6)
    )
    initial = factor / n * (center * identity - matrix) + MODES / n * identity
    edge = jnp.zeros((n, WIDTH - n), jnp.float32)
    initial = jnp.concatenate([initial, edge], axis=1)
    identity = jnp.where(lanes((n, WIDTH)) == sublanes((n, WIDTH)), 1.0, 0.0)
    fill = jnp.zeros((WIDTH - n, WIDTH), jnp.bfloat16)
    empty = jnp.zeros((WIDTH, WIDTH), jnp.bfloat16)

    def step(index, density):
        high, low = [jnp.concatenate([part, fill], axis=0) for part in split(density)]
        weights = jnp.concatenate(
            [jnp.concatenate([high, low], axis=1), jnp.concatenate([high, empty], axis=1)], axis=0
        )

        def times_density(value):
            both = lax.dot_general(
                jnp.concatenate(split(value), axis=1),
                weights,
                (((1,), (0,)), ((), ())),
                preferred_element_type=jnp.float32,
            )
            return both[:, :WIDTH] + both[:, WIDTH:]

        square = times_density(density)
        cube = times_density(square)
        denominator = total((density - square) * identity)
        numerator = total(square * (identity - density))
        safe = jnp.where(jnp.abs(denominator) > 1e-12, denominator, 1.0)
        ratio = jnp.clip(numerator / safe, 0.0, 1.0)
        up = ratio >= 0.5
        scale = 1.0 / jnp.maximum(jnp.where(up, ratio, 1.0 - ratio), 0.5)
        first = jnp.where(up, 0.0, (1.0 - 2.0 * ratio) * scale)
        second = (1.0 + ratio) * scale
        return first * density + second * square - scale * cube

    return lax.fori_loop(0, PURIFY, step, initial)[:MODES, :n]


def pack32(block):
    return jnp.concatenate([block[8 * k : 8 * k + 8] for k in range(4)], axis=1)


def unpack32(tile):
    return jnp.concatenate([tile[:, MODES * k : MODES * (k + 1)] for k in range(4)], axis=0)


def pack64(block):
    return jnp.concatenate([block[:16], block[16:]], axis=1)


def unpack64(tile):
    return jnp.concatenate([tile[:, : 2 * MODES], tile[:, 2 * MODES :]], axis=0)


def pack96(block):
    last = [block[24:, MODES * k : MODES * (k + 1)] for k in range(3)]
    return jnp.concatenate([block[:24], jnp.concatenate(last, axis=0)], axis=1)


def unpack96(tile):
    last = [tile[8 * k : 8 * k + 8, 3 * MODES :] for k in range(3)]
    return jnp.concatenate([tile[:, : 3 * MODES], jnp.concatenate(last, axis=1)], axis=0)


def first_factor(gram_mass):
    return inverse_factor(0.5 * (gram_mass + gram_mass.T), 0)


def next_factor(gram_mass):
    n = gram_mass.shape[0]
    rest = n - MODES
    side = gram_mass[:, :MODES]
    side = jnp.where(sublanes((n, MODES)) < MODES, 0.0, side)
    lower = gram_mass[MODES:, :]
    schur = lower - mm_nt(side[MODES:], side, HIGHEST)
    bottom = inverse_factor(jnp.where(lanes((rest, n)) < MODES, -lower, schur), MODES)
    shape = (MODES, n)
    unit = jnp.where(lanes(shape) == sublanes(shape), 1.0, 0.0)
    return jnp.concatenate([unit, bottom], axis=0)


def ritz_rows(reduced, factor):
    rows = purify(reduced)
    change = inverse_factor(mm_nt(rows, rows, HIGHEST), 0)
    coefficients = mm(rows, factor, HIGHEST)
    projected = mm_nt(mm(rows, reduced, HIGHEST), rows, HIGHEST)
    coefficients = mm(change, coefficients, HIGHEST)
    projected = mm_nt(mm(change, projected, HIGHEST), change, HIGHEST)
    return coefficients, projected


def solve_kernel(
    sizes,
    diag_hbm,
    coupling_hbm,
    offsets_hbm,
    mass_hbm,
    initial_hbm,
    out,
    diag,
    coupling,
    high,
    low,
    mass,
    offsets,
    slot_of,
    inverse_diag,
    product,
    ext0,
    ext1,
    ext2,
    ext3,
    stiff_new,
    modes,
    stiff_modes,
    direction,
    stiff_direction,
    edge,
    landing,
    returned,
    load_sem,
    matrix_sem,
    halo_send,
    halo_recv,
    *channel_refs,
):
    count, blocks = sizes
    ny, nx, cores = TORUS
    side = nx
    me = lax.axis_index("row")
    core = lax.rem(me, cores)
    x = lax.rem(lax.div(me, cores), nx)
    y = lax.div(me, cores * nx)
    partner = me + 1 - 2 * core
    exts = (ext0, ext1, ext2, ext3)
    groups = blocks // REACH

    table_load = pltpu.make_async_copy(offsets_hbm, offsets, load_sem.at[blocks + 1])
    loads = [pltpu.make_async_copy(mass_hbm, mass, load_sem.at[blocks])]
    loads += [
        pltpu.make_async_copy(
            initial_hbm.at[:, pl.ds(b * WIDTH, WIDTH)], ext0.at[b + REACH], load_sem.at[b]
        )
        for b in range(blocks)
    ]
    matrix_loads = [
        [
            pltpu.make_async_copy(
                ref.at[pl.ds(g * REACH, REACH)], out.at[pl.ds(g * REACH, REACH)], matrix_sem.at[i, g]
            )
            for i, (ref, out) in enumerate([(diag_hbm, diag), (coupling_hbm, coupling)])
        ]
        for g in range(groups)
    ]
    table_load.start()
    for copy in loads:
        copy.start()
    for pair in matrix_loads:
        for copy in pair:
            copy.start()

    farthest = sorted(range(1, side), key=lambda k: -min(k, side - k))
    x_at = [lax.rem(x + k, nx) for k in range(side)]
    y_at = [lax.rem(y + k, ny) for k in range(side)]

    def device(px, py, pcore):
        return {"row": (py * nx + px) * cores + pcore}

    barrier = pltpu.get_barrier_semaphore()
    greeted = [{"row": partner}, {"row": lax.rem(me + 1, count)}, {"row": lax.rem(me + count - 1, count)}]
    for k in range(1, side):
        for pcore in range(cores):
            greeted += [device(x_at[k], y, pcore), device(x, y_at[k], pcore)]
    for other in greeted:
        pl.semaphore_signal(barrier, inc=1, device_id=other, device_id_type=MESH)

    def send(source, target, send_sem, recv_sem, other):
        return pltpu.make_async_remote_copy(
            src_ref=source,
            dst_ref=target,
            send_sem=send_sem,
            recv_sem=recv_sem,
            device_id=other,
            device_id_type=MESH,
        )

    def forward(app):
        return send(
            exts[app].at[pl.ds(blocks, REACH)],
            landing.at[app],
            halo_send.at[app, 0],
            halo_recv.at[app, 0],
            {"row": me + 1},
        )

    def backward(app):
        return send(
            edge.at[app],
            returned.at[app],
            halo_send.at[app, 1],
            halo_recv.at[app, 1],
            {"row": me - 1},
        )

    def own_products(ext, b):
        out = mm3(ext[b + REACH], (high[b], low[b]))
        stiff_new[b] = out[:, :WIDTH]
        for s in range(SLOTS):
            product[b, s] = out[:, (s + 1) * WIDTH : (s + 2) * WIDTH]

    def other_products(ext, b):
        taken = jnp.concatenate([ext[b + REACH - offsets[s, b]] for s in range(SLOTS)], axis=1)
        spread = [product[b + d, slot_of[b + d, d - 1]] for d in range(1, REACH + 1)]
        spread = (spread[0] + spread[1]) + (spread[2] + spread[3])
        out = mm3(taken, (high[b, :, WIDTH:], low[b, :, WIDTH:]), True)
        stiff_new[b] = stiff_new[b] + out + spread

    def send_forward(app):
        @pl.when(me < count - 1)
        def _():
            forward(app).start()

    def send_backward(app):
        for e in range(REACH):
            out = jnp.zeros((MODES, WIDTH), jnp.float32)
            for b in range(e + 1):
                out = out + product[b, slot_of[b, b - e + REACH - 1]]
            edge[app, e] = out

        @pl.when(me > 0)
        def _():
            backward(app).start()

    def late_part(app, g):
        return mm3(wide([(exts[app], REACH)], g), wide([(stiff_new, 0)], g), True)

    def rest_of_product(app, ready):
        ext = exts[app]
        for g in range(1, groups):
            ready(g)
            for b in range(g * REACH, (g + 1) * REACH):
                own_products(ext, b)
        for b in range(REACH, blocks):
            other_products(ext, b)
        acc = late_part(app, 1)
        for g in range(2, groups - 1):
            acc = acc + late_part(app, g)

        @pl.when(me > 0)
        def _():
            forward(app).wait_recv()
            ext[0:REACH] = landing[app]

        @pl.when(me == 0)
        def _():
            ext[0:REACH] = jnp.zeros((REACH, MODES, WIDTH), jnp.float32)

        for b in range(REACH):
            other_products(ext, b)
        acc = acc + late_part(app, 0)

        @pl.when(me < count - 1)
        def _():
            backward(app).wait_recv()
            for k in range(REACH):
                b = blocks - REACH + k
                stiff_new[b] = stiff_new[b] + returned[app, k]

        return acc + late_part(app, groups - 1)

    class Channel:
        def __init__(self, refs):
            (self.part, self.first, self.second, self.sends, self.first_sem, self.second_sem) = refs
            self.own_first = (x * (1 - core) + y * core) * cores + core
            self.own_second = y * (1 - core) + x * core

        def first_send(self, half, k):
            if half == 0:
                slot, target = x * cores + core, device(x_at[k], y, 0)
            else:
                slot, target = y * cores + core, device(x, y_at[k], 1)
            return send(
                self.part.at[half],
                self.first.at[slot],
                self.sends.at[0, half, k],
                self.first_sem.at[slot],
                target,
            )

        def first_partner(self):
            half = 1 - core
            slot = (x * core + y * half) * cores + core
            return send(
                self.part.at[half],
                self.first.at[slot],
                self.sends.at[0, half, 0],
                self.first_sem.at[slot],
                {"row": partner},
            )

        def second_send(self, pcore, k):
            where = self.own_second
            px = x * (1 - core) + x_at[k] * core
            py = y_at[k] * (1 - core) + y * core
            return send(
                self.second.at[core, where],
                self.second.at[core, where],
                self.sends.at[1, pcore, k],
                self.second_sem.at[core, where],
                device(px, py, pcore),
            )

        def second_partner(self):
            where = self.own_second
            return send(
                self.second.at[core, where],
                self.second.at[core, where],
                self.sends.at[1, 1 - core, 0],
                self.second_sem.at[core, where],
                {"row": partner},
            )

        def arrived(self, buffer, sem, index):
            send(
                buffer.at[index], buffer.at[index], self.sends.at[0, 0, 0], sem.at[index],
                {"row": partner},
            ).wait_recv()

        def store(self, packed):
            rows = packed.shape[0] // 2
            self.part[0] = packed[:rows]
            self.part[1] = packed[rows:]

        def start(self):
            self.first[self.own_first] = self.part[core]
            for k in farthest:
                for half in range(2):
                    self.first_send(half, k).start()
            self.first_partner().start()

        def middle(self):
            slots = side * cores
            for k in range(1, slots):
                self.arrived(self.first, self.first_sem, lax.rem(self.own_first + k, slots))
            values = [self.first[k] for k in range(slots)]
            while len(values) > 1:
                values = [p + q for p, q in zip(values[::2], values[1::2])]
            self.second[core, self.own_second] = values[0]
            for k in farthest:
                for pcore in range(cores):
                    self.second_send(pcore, k).start()
            self.second_partner().start()

        def finish(self):
            for k in range(1, side):
                self.arrived(
                    self.second, self.second_sem, (core, lax.rem(self.own_second + k, side))
                )
            for k in range(side):
                self.arrived(self.second, self.second_sem, (1 - core, k))
            halves = []
            for half in range(2):
                values = [self.second[half, k] for k in range(side)]
                while len(values) > 1:
                    values = [p + q for p, q in zip(values[::2], values[1::2])]
                halves.append(values[0])
            return jnp.concatenate(halves, axis=0)

        def drain(self):
            for k in range(1, side):
                for half in range(2):
                    self.first_send(half, k).wait_send()
                    self.second_send(half, k).wait_send()
            self.first_partner().wait_send()
            self.second_partner().wait_send()

    channels, taken = [], 0
    for tiles in CHANNELS:
        channels.append([])
        for _ in tiles:
            channels[-1].append(Channel(channel_refs[taken : taken + 6]))
            taken += 6

    def drain(app):
        @pl.when(me < count - 1)
        def _():
            forward(app).wait_send()

        @pl.when(me > 0)
        def _():
            backward(app).wait_send()

        for channel in channels[app]:
            channel.drain()

    def wide(refs, group):
        return jnp.concatenate(
            [
                jnp.concatenate([ref[group * REACH + k + shift] for ref, shift in refs], axis=0)
                for k in range(REACH)
            ],
            axis=1,
        )

    def wide_row(ref, group):
        return jnp.concatenate(
            [ref[group * REACH + k : group * REACH + k + 1, :] for k in range(REACH)], axis=1
        )

    for b in range(blocks + REACH):
        product[b, SLOTS] = jnp.zeros((MODES, WIDTH), jnp.float32)
    for copy in loads:
        copy.wait()
    acc = jnp.zeros((MODES, MODES), jnp.float32)
    for g in range(groups):
        left = wide([(ext0, REACH)], g)
        acc = acc + mm3(left * wide_row(mass, g), left, True)
    channels[0][0].store(pack32(acc))
    table_load.wait()
    for b in range(blocks):
        for d in range(1, REACH + 1):
            slot = SLOTS
            for s in range(SLOTS):
                slot = jnp.where(offsets[s, b] == d, s, slot)
            slot_of[b, d - 1] = slot
    for b in range(blocks, blocks + REACH):
        for d in range(REACH):
            slot_of[b, d] = SLOTS

    def ready(g):
        for copy in matrix_loads[g]:
            copy.wait()
        for b in range(g * REACH, (g + 1) * REACH):
            whole = jnp.concatenate([diag[b]] + [coupling[b, s] for s in range(SLOTS)], axis=1)
            high[b], low[b] = split(whole)

    ready(0)
    for b in range(REACH):
        own_products(ext0, b)
    pl.semaphore_wait(barrier, len(greeted))
    send_forward(0)
    send_backward(0)
    channels[0][0].start()
    channels[0][1].store(pack32(rest_of_product(0, ready)))
    channels[0][1].start()
    identity = eye(WIDTH)
    for b in range(blocks):
        inverse_diag[b : b + 1, :] = 1.0 / jnp.sum(diag[b] * identity, axis=0, keepdims=True)
    channels[0][0].middle()
    channels[0][1].middle()
    factor = first_factor(unpack32(channels[0][0].finish()))
    block = unpack32(channels[0][1].finish())
    projected = mm_nt(mm(factor, block, HIGHEST), factor, HIGHEST)
    projected = 0.5 * (projected + projected.T)
    coefficients = factor
    basis, stiff_basis = [(ext0, REACH)], [(stiff_new, 0)]
    previous = None

    for step in range(1, ITERS + 1):
        ext = exts[step]
        order = coefficients.shape[1]
        later = jnp.where(lanes((MODES, order)) < MODES, 0.0, coefficients)
        moving = previous is not None
        both = jnp.concatenate([coefficients, later], axis=0) if moving else coefficients
        n = MODES * (3 if moving else 2)
        stiff_acc = jnp.zeros((MODES, n - MODES), jnp.float32)
        mass_acc = jnp.zeros((MODES, n), jnp.float32)
        for g in (groups - 1, 0, *range(1, groups - 1)):
            new = mm3(both, wide(basis, g))
            stiff = mm3(both, wide(stiff_basis, g))
            masses = wide_row(mass, g)
            residual = stiff[:MODES] - mm3(projected, new[:MODES] * masses)
            residual = residual * wide_row(inverse_diag, g)
            for k in range(REACH):
                b = g * REACH + k
                cut = slice(k * WIDTH, (k + 1) * WIDTH)
                modes[b] = new[:MODES, cut]
                stiff_modes[b] = stiff[:MODES, cut]
                ext[b + REACH] = residual[:, cut]
                if moving:
                    direction[b] = new[MODES:, cut]
                    stiff_direction[b] = stiff[MODES:, cut]
            right = [new[:MODES], residual] + ([new[MODES:]] if moving else [])
            mass_acc = mass_acc + mm3(residual * masses, jnp.concatenate(right, axis=0), True)
            stiff_acc = stiff_acc + mm3(residual, stiff, True)
            if g == 0:
                for b in range(REACH):
                    own_products(ext, b)
                send_forward(step)
                send_backward(step)
        early_sum, late_sum = channels[step]
        packed = [pack96(mass_acc), pack64(stiff_acc)] if moving else [pack64(mass_acc), pack32(stiff_acc)]
        early_sum.store(jnp.concatenate(packed, axis=0))
        early_sum.start()
        late_sum.store(pack32(rest_of_product(step, lambda g: None)))
        late_sum.start()
        basis = [(modes, 0), (ext, REACH)] + ([(direction, 0)] if moving else [])
        stiff_basis = [(stiff_modes, 0), (stiff_new, 0)] + ([(stiff_direction, 0)] if moving else [])
        shape = (MODES, n)
        lane = lanes(shape)
        unit = jnp.where(lane == sublanes(shape), 1.0, 0.0)
        placed = mm(0.5 * projected, unit, HIGHEST)
        third = []
        if moving:
            zero = jnp.zeros((MODES, order), jnp.float32)
            spread_rows = jnp.concatenate([coefficients, zero, later], axis=0)
            third = [
                [
                    mm_nt(mm(later, old, HIGHEST), spread_rows, HIGHEST)
                    * jnp.where(lane < 2 * MODES, 1.0, 0.5)
                ]
                for old in previous
            ]
        else:
            third = [[], []]
        drain(step - 1)
        early_sum.middle()
        late_sum.middle()
        early = early_sum.finish()
        early_mass = unpack96(early[:24]) if moving else unpack64(early[:16])
        half = jnp.where((lane >= MODES) & (lane < 2 * MODES), 0.5, 1.0)
        gram_mass = jnp.concatenate([0.5 * unit, early_mass * half] + third[1], axis=0)
        gram_mass = gram_mass + gram_mass.T
        factor = next_factor(gram_mass)
        middle = factor[:, MODES : 2 * MODES]
        early_stiff = unpack64(early[24:]) if moving else unpack32(early[16:])
        empty = jnp.zeros((MODES, MODES), jnp.float32)
        pieces = [early_stiff[:, :MODES], empty] + ([early_stiff[:, MODES:]] if moving else [])
        rest = jnp.concatenate([placed, jnp.concatenate(pieces, axis=1)] + third[0], axis=0)
        rest = rest + rest.T
        known = mm_nt(mm(factor, rest, HIGHEST), factor, HIGHEST)
        tile = late_sum.finish()
        block = unpack32(tile)
        reduced = known + mm_nt(mm(middle, block, HIGHEST), middle, HIGHEST)
        coefficients, projected = ritz_rows(reduced, factor)
        if step < ITERS:
            block_lane = lanes((8, WIDTH))
            here = (block_lane >= MODES) & (block_lane < 2 * MODES)
            turned = [tile if k == 1 else pltpu.roll(tile, (1 - k) % 4 * MODES, 1) for k in range(4)]
            inner = jnp.concatenate([jnp.where(here, t, 0.0) for t in turned], axis=0)[:, :n]
            empty = jnp.zeros((MODES, n), jnp.float32)
            inner = jnp.concatenate([empty, inner] + [empty] * (n // MODES - 2), axis=0)
            previous = [rest + inner, gram_mass]

    for g in range(groups):
        new = mm3(coefficients, wide(basis, g))
        stiff = mm3(coefficients, wide(stiff_basis, g))
        squares = jnp.sum(new * new, axis=0, keepdims=True)
        energy = jnp.sum(new * stiff, axis=0, keepdims=True)
        for k in range(REACH):
            cut = slice(k * WIDTH, (k + 1) * WIDTH)
            b = g * REACH + k
            out[0, b : b + 1, :] = squares[:, cut]
            out[1, b : b + 1, :] = energy[:, cut]
    drain(ITERS)


def solution(mesh):
    count = mesh.shape["row"]

    def local(diag_blocks, coupling, offsets, mass, initial_modes):
        blocks = diag_blocks.shape[0]
        apps = ITERS + 1
        side = TORUS[1]
        cores = TORUS[2]
        f32 = jnp.float32
        dma = pltpu.SemaphoreType.DMA
        vector = pltpu.VMEM((blocks, MODES, WIDTH), f32)
        extended = pltpu.VMEM((blocks + REACH, MODES, WIDTH), f32)
        halo = pltpu.VMEM((apps, REACH, MODES, WIDTH), f32)
        channel_shapes = []
        for tiles in CHANNELS:
            for tile in tiles:
                rows = 4 * tile
                channel_shapes += [
                    pltpu.VMEM((2, rows, WIDTH), f32),
                    pltpu.VMEM((side * cores, rows, WIDTH), f32),
                    pltpu.VMEM((2, side, rows, WIDTH), f32),
                    dma((2, 2, side)),
                    dma((side * cores,)),
                    dma((2, side)),
                ]
        sums = pl.pallas_call(
            lambda *refs: solve_kernel((count, blocks), *refs),
            out_shape=jax.ShapeDtypeStruct((2, blocks, WIDTH), f32),
            in_specs=[
                pl.BlockSpec(memory_space=pltpu.HBM),
                pl.BlockSpec(memory_space=pltpu.HBM),
                pl.BlockSpec(memory_space=pltpu.HBM),
                pl.BlockSpec(memory_space=pltpu.HBM),
                pl.BlockSpec(memory_space=pltpu.HBM),
            ],
            out_specs=pl.BlockSpec(memory_space=pltpu.VMEM),
            scratch_shapes=[
                pltpu.VMEM((blocks, WIDTH, WIDTH), f32),
                pltpu.VMEM((blocks, SLOTS, WIDTH, WIDTH), f32),
                pltpu.VMEM((blocks, WIDTH, (SLOTS + 1) * WIDTH), jnp.bfloat16),
                pltpu.VMEM((blocks, WIDTH, (SLOTS + 1) * WIDTH), jnp.bfloat16),
                pltpu.VMEM((blocks, WIDTH), f32),
                pltpu.SMEM((SLOTS, blocks), jnp.int32),
                pltpu.SMEM((blocks + REACH, REACH), jnp.int32),
                pltpu.VMEM((blocks, WIDTH), f32),
                pltpu.VMEM((blocks + REACH, SLOTS + 1, MODES, WIDTH), f32),
                extended,
                extended,
                extended,
                extended,
                vector,
                vector,
                vector,
                vector,
                vector,
                halo,
                halo,
                halo,
                dma((blocks + 2,)),
                dma((2, blocks // REACH)),
                dma((apps, 2)),
                dma((apps, 2)),
                *channel_shapes,
            ],
            compiler_params=pltpu.CompilerParams(
                collective_id=0, has_side_effects=True, vmem_limit_bytes=56 << 20
            ),
            name="lobpcg",
        )(diag_blocks, coupling, offsets.T, mass.reshape(blocks, WIDTH), initial_modes)
        weight = count * blocks * WIDTH / MODES
        return weight * mass * sums[0].reshape(-1), weight * sums[1].reshape(-1)

    spec = ("sub", "row")
    return jax.shard_map(
        local,
        mesh=mesh,
        in_specs=(
            P(spec, None, None),
            P(spec, None, None, None),
            P(spec, None),
            P(spec),
            P(None, spec),
        ),
        out_specs=(P(spec), P(spec)),
        check_vma=False,
    )
```
